16 devices in a mesh: rep: 4 (over y, z, core), dp: 4 (over x).
Axes of the slice: x: 4, y: 2, z: 1, core: 2. Of those that a mesh axis runs over, the one named last changes fastest.
The devices are a block of a 4x4x8 slice.
Arguments:
- x: bfloat16 [16, 2048, 640], P(('rep', 'dp')), parts along dimension 0
- dy: bfloat16 [16, 2048, 640], P(('rep', 'dp')), parts along dimension 0
- wq: bfloat16 [2, 640, 1536], P(None, 'dp')
- wk: bfloat16 [2, 640, 128], P(None, 'dp')
- wv: bfloat16 [2, 640, 128], P(None, 'dp')
- wo: bfloat16 [2, 1536, 640], P(None, 'dp')
- w_gate: bfloat16 [2, 640, 1536], P(None, 'dp')
- w_up: bfloat16 [2, 640, 1536], P(None, 'dp')
- w_down: bfloat16 [2, 1536, 640], P(None, 'dp')
- m_wq: float32 [2, 640, 1536], P(None, 'dp')
- m_wk: float32 [2, 640, 128], P(None, 'dp')
- m_wv: float32 [2, 640, 128], P(None, 'dp')
- m_wo: float32 [2, 1536, 640], P(None, 'dp')
- m_w_gate: float32 [2, 640, 1536], P(None, 'dp')
- m_w_up: float32 [2, 640, 1536], P(None, 'dp')
- m_w_down: float32 [2, 1536, 640], P(None, 'dp')
- v_wq: float32 [2, 640, 1536], P(None, 'dp')
- v_wk: float32 [2, 640, 128], P(None, 'dp')
- v_wv: float32 [2, 640, 128], P(None, 'dp')
- v_wo: float32 [2, 1536, 640], P(None, 'dp')
- v_w_gate: float32 [2, 640, 1536], P(None, 'dp')
- v_w_up: float32 [2, 640, 1536], P(None, 'dp')
- v_w_down: float32 [2, 1536, 640], P(None, 'dp')
Outputs:
- output 1: bfloat16 [8, 640, 1536], P('rep', 'dp'), parts along dimension 0
- output 2: bfloat16 [8, 640, 128], P('rep', 'dp'), parts along dimension 0
- output 3: bfloat16 [8, 640, 128], P('rep', 'dp'), parts along dimension 0
- output 4: bfloat16 [8, 1536, 640], P('rep', 'dp'), parts along dimension 0
- output 5: bfloat16 [8, 640, 1536], P('rep', 'dp'), parts along dimension 0
- output 6: bfloat16 [8, 640, 1536], P('rep', 'dp'), parts along dimension 0
- output 7: bfloat16 [8, 1536, 640], P('rep', 'dp'), parts along dimension 0
- output 8: float32 [8, 640, 1536], P('rep', 'dp'), parts along dimension 0
- output 9: float32 [8, 640, 128], P('rep', 'dp'), parts along dimension 0
- output 10: float32 [8, 640, 128], P('rep', 'dp'), parts along dimension 0
- output 11: float32 [8, 1536, 640], P('rep', 'dp'), parts along dimension 0
- output 12: float32 [8, 640, 1536], P('rep', 'dp'), parts along dimension 0
- output 13: float32 [8, 640, 1536], P('rep', 'dp'), parts along dimension 0
- output 14: float32 [8, 1536, 640], P('rep', 'dp'), parts along dimension 0
- output 15: float32 [8, 640, 1536], P('rep', 'dp'), parts along dimension 0
- output 16: float32 [8, 640, 128], P('rep', 'dp'), parts along dimension 0
- output 17: float32 [8, 640, 128], P('rep', 'dp'), parts along dimension 0
- output 18: float32 [8, 1536, 640], P('rep', 'dp'), parts along dimension 0
- output 19: float32 [8, 640, 1536], P('rep', 'dp'), parts along dimension 0
- output 20: float32 [8, 640, 1536], P('rep', 'dp'), parts along dimension 0
- output 21: float32 [8, 1536, 640], P('rep', 'dp'), parts along dimension 0
There are 4 independent parts. The reference program is written for one: setup_inputs(seed, part) draws one part's arguments, and reference() takes and returns one part's arrays. A program takes and returns all parts, laid end to end along the dimension named above; an argument that names none is the same for every part.
All inputs are finite; a program needn't handle non-finite values.
Results may differ from the reference program's by a relative error of at most 0.0307.
Values are sent between devices in bfloat16 or wider.
A program may use at most 768 MiB of HBM per device.

```python
import jax
import jax.numpy as jnp
from jax import lax

SEQUENCES = 4
TOKENS = 2048
D = 640
HEADS = 12
KV_HEADS = 1
HEAD = 128
FF = 1536
LAYERS = 2
THETA = 10000
NAMES = ("wq", "wk", "wv", "wo", "w_gate", "w_up", "w_down")
SHAPES = {
    "wq": (LAYERS, D, HEADS * HEAD),
    "wk": (LAYERS, D, KV_HEADS * HEAD),
    "wv": (LAYERS, D, KV_HEADS * HEAD),
    "wo": (LAYERS, HEADS * HEAD, D),
    "w_gate": (LAYERS, D, FF),
    "w_up": (LAYERS, D, FF),
    "w_down": (LAYERS, FF, D),
}


def bump(key, n, height):
    away = (jnp.arange(n, dtype=jnp.int32) - jax.random.randint(key, (), 0, n, jnp.int32)) % n
    return jnp.where(away < n // 8, height, 1.0)


def together(key, own, strength):
    shared = jax.random.normal(key, own.shape[1:], jnp.float32)
    return (own + strength * shared) * lax.rsqrt(1 + strength * strength)


def setup_inputs(seed: int = 0, part: int = 0) -> dict:
    kx, kdy, ka, kb, kz, kf, kh, kl, *keys = jax.random.split(jax.random.key(seed), 8 + 3 * len(NAMES))
    kx, kdy, ka, kb = (jax.random.fold_in(k, part) for k in (kx, kdy, ka, kb))
    kw, km, kv = (keys[i::3] for i in range(3))
    shape = (SEQUENCES, TOKENS, D)
    much_x, much_dy = jax.random.uniform(kz, (2,), jnp.float32, 0.0, 1.0)
    loud = 2.0 ** jax.random.uniform(jax.random.fold_in(kz, 1), (), jnp.float32, -1.0, 2.0)
    layers = 2.0 ** jax.random.uniform(kl, (LAYERS, 1, 1), jnp.float32, -1.0, 1.0)
    times = {"wq": 1.0, "wk": 1.0, "wv": 2.0, "wo": layers, "w_gate": 1.0, "w_up": bump(kh, FF, 4.0), "w_down": layers}
    x = together(ka, jax.random.normal(kx, shape, jnp.float32), much_x) * bump(kf, D, 4.0)
    dy = together(kb, jax.random.normal(kdy, shape, jnp.float32), much_dy)
    drawn = {"x": x.astype(jnp.bfloat16), "dy": (loud * dy * (SEQUENCES * TOKENS) ** -0.5).astype(jnp.bfloat16)}
    for key, name in zip(kw, NAMES, strict=True):
        drawn[name] = (jax.random.normal(key, SHAPES[name], jnp.float32) * SHAPES[name][1] ** -0.5 * times[name]).astype(jnp.bfloat16)
    for key, name in zip(km, NAMES, strict=True):
        drawn[f"m_{name}"] = 0.1 * jax.random.normal(key, SHAPES[name], jnp.float32)
    for key, name in zip(kv, NAMES, strict=True):
        drawn[f"v_{name}"] = jax.random.uniform(key, SHAPES[name], jnp.float32, 0.02, 0.06)
    return drawn


def matmul(a, w):
    return jnp.dot(a, w, preferred_element_type=jnp.float32).astype(jnp.bfloat16)


def normed(h):
    wide = h.astype(jnp.float32)
    scale = lax.rsqrt(jnp.mean(wide**2, -1, keepdims=True) + 1e-6)
    return (wide * scale).astype(jnp.bfloat16)


def turned(t, theta):
    half = t.shape[-1] // 2
    angle = jnp.arange(t.shape[0], dtype=jnp.float32)[:, None] * theta ** (-jnp.arange(half, dtype=jnp.float32) / half)
    cos, sin = jnp.cos(angle)[:, None], jnp.sin(angle)[:, None]
    a, b = t[..., :half].astype(jnp.float32), t[..., half:].astype(jnp.float32)
    return jnp.concatenate([a * cos - b * sin, b * cos + a * sin], -1).astype(jnp.bfloat16)


def seen_by(q, k, v):
    tokens, kv = q.shape[0], k.shape[1]
    q = q.reshape(tokens, kv, -1, q.shape[-1])
    scores = jnp.einsum("tgsd,ugd->gstu", q.astype(jnp.float32), k.astype(jnp.float32)) * q.shape[-1] ** -0.5
    place = jnp.arange(tokens)
    weights = jax.nn.softmax(jnp.where(place[:, None] >= place, scores, -jnp.inf), -1).astype(jnp.bfloat16)
    return jnp.einsum("gstu,ugd->tgsd", weights.astype(jnp.float32), v.astype(jnp.float32)).astype(jnp.bfloat16).reshape(tokens, -1)


def layer(h, w):
    a = normed(h)
    q, k = (turned(matmul(a, w[name]).reshape(h.shape[0], -1, HEAD), THETA) for name in ("wq", "wk"))
    h = h + matmul(seen_by(q, k, matmul(a, w["wv"]).reshape(h.shape[0], -1, HEAD)), w["wo"])
    b = normed(h)
    gate = jnp.dot(b, w["w_gate"], preferred_element_type=jnp.float32)
    up = jnp.dot(b, w["w_up"], preferred_element_type=jnp.float32)
    return h + matmul((jax.nn.silu(gate) * up).astype(jnp.bfloat16), w["w_down"])


def adamw(w, m, v, g):
    m = 0.9 * m + 0.1 * g
    v = 0.95 * v + 0.05 * g * g
    step = m * lax.rsqrt(v + 1e-8) + 0.1 * w
    return (w - 0.02 * step).astype(jnp.bfloat16), m, v


def clipped(gradients, sum_of_squares, count):
    factor = jnp.minimum(1.0, 0.5 * lax.rsqrt(sum_of_squares / count + 1e-30))
    return [g * factor for g in gradients]


def stack(weights, h):
    return lax.scan(lambda h, w: (layer(h, w), None), h, weights)[0]


def reference(x, dy, wq, wk, wv, wo, w_gate, w_up, w_down, m_wq, m_wk, m_wv, m_wo, m_w_gate, m_w_up, m_w_down, v_wq, v_wk, v_wv, v_wo, v_w_gate, v_w_up, v_w_down):
    weights = dict(zip(NAMES, (wq, wk, wv, wo, w_gate, w_up, w_down), strict=True))

    def take(so_far, sequence):
        h, by_y = sequence
        _, back = jax.vjp(stack, weights, h)
        by_weights, by_h = back(by_y)
        return jax.tree.map(lambda total, term: total + term.astype(jnp.float32), so_far, by_weights), by_h

    none_yet = {name: jnp.zeros(w.shape, jnp.float32) for name, w in weights.items()}
    by_weights, by_x = lax.scan(take, none_yet, (x, dy))
    gradients = [by_weights[name].astype(jnp.bfloat16).astype(jnp.float32) for name in NAMES]
    gradients = clipped(gradients, sum(jnp.sum(g * g) for g in gradients), sum(g.size for g in gradients))
    first = (m_wq, m_wk, m_wv, m_wo, m_w_gate, m_w_up, m_w_down)
    second = (v_wq, v_wk, v_wv, v_wo, v_w_gate, v_w_up, v_w_down)
    new = [adamw(weights[name].astype(jnp.float32), m, v, g) for name, m, v, g in zip(NAMES, first, second, gradients, strict=True)]
    return tuple(one[which] for which in range(3) for one in new)
```

```python
import functools
import itertools

import jax
import jax.numpy as jnp
from jax import lax
from jax.experimental import pallas as pl
from jax.experimental.pallas import tpu as pltpu
from jax.sharding import PartitionSpec as P

HEAD = 128
THETA = 10000
NAMES = ("wq", "wk", "wv", "wo", "w_gate", "w_up", "w_down")
NEG = -1e30
HIDDEN = 2 * NEG
LOG2E = 1.4426950408889634
VMEM = 60 * 2**20
F32, BF16 = jnp.float32, jnp.bfloat16


def _mm(a, b, ca=1, cb=0):
    return lax.dot_general(a, b, (((ca,), (cb,)), ((), ())), preferred_element_type=F32)


def _fit(size, want, unit=128):
    return max(n for n in range(unit, max(min(want, size), unit) + 1, unit) if size % n == 0)


def _normed(h):
    wide = h.astype(F32)
    scale = lax.rsqrt(jnp.mean(wide * wide, -1, keepdims=True) + 1e-6)
    return wide, scale, (wide * scale).astype(BF16)


def _norm_back(wide, scale, by_a):
    by_a = by_a.astype(BF16).astype(F32)
    along = jnp.sum(by_a * wide, -1, keepdims=True) * (scale * scale * scale) * (1 / wide.shape[-1])
    return (by_a * scale - wide * along).astype(BF16)


def _plus(a, b):
    return (a.astype(F32) + b.astype(BF16).astype(F32)).astype(BF16)


def _turned(t, cos, sin):
    t = t.astype(BF16).astype(F32)
    return (t * cos + pltpu.roll(t, t.shape[1] // 2, 1) * sin).astype(BF16)


MESH = pl.DeviceIdType.MESH


class Gather:
    def __init__(self, number, arrays, when):
        self.number, self.arrays, self.when = number, arrays, when

    def ins(self):
        return [(a, None) for a in self.arrays]

    def outs(self, n):
        return [(n * a.shape[0], a.shape[1]) for a in self.arrays]

    def scratch(self):
        return [pltpu.SemaphoreType.DMA((len(self.arrays), 3))] * 4 + [pltpu.SemaphoreType.DMA((len(self.arrays),))]

    def run(self, step, last, shards, wholes, scratch, before):
        send, come, give, get, own = scratch
        me, rep, n = lax.axis_index("dp"), lax.axis_index("rep"), lax.axis_size("dp")
        core = lax.rem(rep, 2)
        partner = rep + 1 - 2 * core

        def rows(i, owner, half):
            size = shards[i].shape[0] // 2
            return pl.ds(pl.multiple_of((2 * owner + half) * size, size), size)

        def out(i, d):
            half = shards[i].shape[0] // 2
            return pltpu.make_async_remote_copy(
                src_ref=shards[i].at[pl.ds(pl.multiple_of(core * half, half), half), :], dst_ref=wholes[i].at[rows(i, me, core), :],
                send_sem=send.at[i, d - 1], recv_sem=come.at[i, d - 1], device_id={"dp": lax.rem(me + d, n)}, device_id_type=MESH)

        def over(i, d):
            where = rows(i, lax.rem(me + n - d, n), core)
            return pltpu.make_async_remote_copy(
                src_ref=wholes[i].at[where, :], dst_ref=wholes[i].at[where, :],
                send_sem=give.at[i, d - 1], recv_sem=get.at[i, d - 1], device_id={"rep": partner}, device_id_type=MESH)

        def mine(i):
            size = shards[i].shape[0]
            return pltpu.make_async_copy(shards[i], wholes[i].at[pl.ds(pl.multiple_of(me * size, size), size), :], own.at[i])

        all_ = [(i, d) for i in range(len(shards)) for d in range(1, n)]
        if before:

            @pl.when(step == 0)
            def _():
                barrier = pltpu.get_barrier_semaphore()
                for d in range(1, n):
                    pl.semaphore_signal(barrier, inc=1, device_id={"dp": lax.rem(me + d, n)}, device_id_type=MESH)
                pl.semaphore_signal(barrier, inc=1, device_id={"rep": partner}, device_id_type=MESH)
                pl.semaphore_wait(barrier, n)
                for i, d in all_:
                    out(i, d).start()
                for i in range(len(shards)):
                    mine(i).start()

        for at in sorted(set(self.when)):
            if before == (at >= 0):

                @pl.when(step == (at if at >= 0 else last))
                def _():
                    for i, d in all_:
                        if self.when[i] == at:
                            out(i, d).wait_recv()
                            over(i, d).start()

        if not before:

            @pl.when(step == last)
            def _():
                for i, d in all_:
                    out(i, d).wait_send()
                    over(i, d).wait()
                for i in range(len(shards)):
                    mine(i).wait()


class Scatter:
    def __init__(self, number, arrays):
        self.number, self.arrays = number, arrays

    def ins(self):
        return [(a, pltpu.HBM) for a in self.arrays]

    def outs(self, n):
        return [(n - 1, a.shape[0] // n, a.shape[1]) for a in self.arrays]

    def scratch(self):
        return [pltpu.SemaphoreType.DMA((len(self.arrays), 3))] * 2

    def run(self, step, last, terms, comes, scratch, before):
        send, come = scratch
        me, n = lax.axis_index("dp"), lax.axis_size("dp")

        def out(i, d):
            to = lax.rem(me + d, n)
            size = terms[i].shape[0] // n
            return pltpu.make_async_remote_copy(
                src_ref=terms[i].at[pl.ds(pl.multiple_of(to * size, size), size), :], dst_ref=comes[i].at[d - 1],
                send_sem=send.at[i, d - 1], recv_sem=come.at[i, d - 1], device_id={"dp": to}, device_id_type=MESH)

        all_ = [(i, d) for i in range(len(terms)) for d in range(1, n)]

        if before:

            @pl.when(step == 0)
            def _():
                barrier = pltpu.get_barrier_semaphore()
                for d in range(1, n):
                    pl.semaphore_signal(barrier, inc=1, device_id={"dp": lax.rem(me + d, n)}, device_id_type=MESH)
                pl.semaphore_wait(barrier, n - 1)
                for i, d in all_:
                    out(i, d).start()

        else:

            @pl.when(step == last)
            def _():
                for i, d in all_:
                    out(i, d).wait()


def _call(kernel, grid, ins, outs, scratch, flops, exp=0, beside=None):
    whole = lambda a: pl.BlockSpec(a.shape, lambda *_: (0,) * a.ndim, pipeline_mode=pl.Buffered(1))
    spec = lambda i: whole(i[0]) if i[1] is None else pl.BlockSpec(memory_space=i[1]) if i[1] is pltpu.HBM else pl.BlockSpec(i[1], i[2])
    size = sum(i[0].size * i[0].dtype.itemsize for i in ins)
    out_specs = [pl.BlockSpec(o[2], o[3]) for o in outs]
    shapes = [jax.ShapeDtypeStruct(o[0], o[1]) for o in outs]
    body, more = kernel, {}
    if beside is not None:
        more = dict(collective_id=beside.number, has_side_effects=True)
        counts = [len(ins), len(beside.arrays), len(outs), len(beside.arrays), len(scratch)]
        ins = ins + beside.ins()
        shapes += [jax.ShapeDtypeStruct(o, BF16) for o in beside.outs(lax.axis_size("dp"))]
        out_specs += [pl.BlockSpec(memory_space=pltpu.HBM)] * len(beside.arrays)
        scratch = scratch + beside.scratch()

        def body(*refs):
            split, at = [], 0
            for c in counts:
                split.append(refs[at : at + c])
                at += c
            step, last = pl.program_id(0), pl.num_programs(0) - 1
            beside.run(step, last, split[1], split[3], refs[at:], True)
            kernel(*split[0], *split[2], *split[4])
            beside.run(step, last, split[1], split[3], refs[at:], False)

    return pl.pallas_call(
        body,
        grid=grid,
        in_specs=[spec(i) for i in ins],
        out_specs=out_specs,
        out_shape=shapes,
        scratch_shapes=scratch,
        compiler_params=pltpu.CompilerParams(dimension_semantics=("arbitrary",) * len(grid), vmem_limit_bytes=VMEM, **more),
        cost_estimate=pl.CostEstimate(flops=flops, transcendentals=exp, bytes_accessed=2 * size),
    )(*[i[0] for i in ins])


def alone(beside):
    return _call(lambda: None, (1,), [], [], [], 0, beside=beside)


def _qkv(h_ref, w_ref, cos_ref, sin_ref, q_ref, k_ref, v_ref):
    a = _normed(h_ref[...])[2]
    cos, sin = cos_ref[...], sin_ref[...]
    heads = q_ref.shape[0]
    for n in range(0, heads + 2, 2):
        y = _mm(a, w_ref[:, n * HEAD : (n + 2) * HEAD])
        for at in range(n, n + 2):
            part = y[:, (at - n) * HEAD : (at - n + 1) * HEAD]
            if at < heads:
                q_ref[at] = _turned(part, cos, sin)
            elif at == heads:
                k_ref[...] = _turned(part, cos, sin)
            else:
                v_ref[...] = part.astype(BF16)


def qkv(h, w, cos, sin):
    t, d = h.shape
    heads = w.shape[1] // HEAD - 2
    bt = _fit(t, 512)
    rows = lambda i: (i, 0)
    return _call(
        _qkv, (t // bt,),
        [(h, (bt, d), rows), (w, None), (cos, (bt, HEAD), rows), (sin, (bt, HEAD), rows)],
        [((heads, t, HEAD), BF16, (heads, bt, HEAD), lambda i: (0, i, 0)), ((t, HEAD), BF16, (bt, HEAD), rows), ((t, HEAD), BF16, (bt, HEAD), rows)],
        [], 2 * t * d * w.shape[1],
    )


def _spans(iq, bq, bk, block):
    lax.fori_loop(0, lax.div(iq * bq, bk), lambda j, _: block(j * bk, bk, False), None)
    rest = lax.rem(iq, bk // bq)
    for n in range(bk // bq):

        @pl.when(rest == n)
        def _():
            block((iq - n) * bq, (n + 1) * bq, True)


def _level(size, wide, bq):
    return (lax.broadcasted_iota(jnp.int32, (size, wide), 0) - lax.rem(lax.broadcasted_iota(jnp.int32, (size, wide), 1), bq)) <= size - bq


def _attend(q_ref, k_ref, v_ref, o_ref, lse_ref, top_s, mix_s, *, bk, wide):
    g, bq, d = q_ref.shape
    cols = g * bq
    iq = pl.program_id(0)
    scale = d**-0.5
    e = scale * LOG2E
    pieces = range(0, cols, wide)
    top_s[...] = jnp.full((1, cols), NEG, F32)
    mix_s[...] = jnp.zeros((d + 8, cols), F32)

    def block(at_key, size, masked):
        here = pl.ds(pl.multiple_of(at_key, bq), size)
        keys = k_ref[here, :]
        values = jnp.concatenate([v_ref[here, :].T, jnp.ones((8, size), BF16)], axis=0)
        scores = [_mm(keys, q_ref[...].reshape(cols, d)[at : at + wide, :], 1, 1) for at in pieces]
        ok = _level(size, wide, bq) if masked else None
        weights, keeps = [], []
        for at, s in zip(pieces, scores):
            if masked:
                s = jnp.where(ok, s, HIDDEN)
            old = top_s[:, at : at + wide]
            top = jnp.maximum(old, s.max(axis=0, keepdims=True))
            top_s[:, at : at + wide] = top
            weights.append(jnp.exp2((s - top) * e).astype(BF16))
            keeps.append(jnp.exp2((old - top) * e))
        for at, p, keep in zip(pieces, weights, keeps):
            mix_s[:, at : at + wide] = mix_s[:, at : at + wide] * keep + _mm(values, p)

    _spans(iq, bq, bk, block)
    for n in range(g):
        at = slice(n * bq, (n + 1) * bq)
        total = mix_s[d : d + 1, at]
        o_ref[:, n * d : (n + 1) * d] = (mix_s[:d, at] * (1 / total)).T.astype(BF16)
        lse_ref[n : n + 1, :] = top_s[:, at] * scale + jnp.log(total)


def attend(q, k, v, beside):
    g, t, d = q.shape
    bq = _fit(t, 256)
    bk = _fit(t, 512)
    wide = _fit(g * bq, 512, bq)
    rows = lambda i: (i, 0)
    return _call(
        functools.partial(_attend, bk=bk, wide=wide), (t // bq,),
        [(q, (g, bq, d), lambda i: (0, i, 0)), (k, None), (v, None)],
        [((t, g * d), BF16, (bq, g * d), rows), ((g, t), F32, (g, bq), lambda i: (0, i))],
        [pltpu.VMEM((1, g * bq), F32), pltpu.VMEM((d + 8, g * bq), F32)],
        2 * g * t * t * d, g * t * t // 2, beside,
    )


def _out_back(by_h_ref, wo_ref, o_ref, do_ref, delta_ref, by_w_ref, sum_s):
    by_h = by_h_ref[...]
    heads = o_ref.shape[1] // HEAD

    @pl.when(pl.program_id(0) == 0)
    def _():
        sum_s[...] = jnp.zeros_like(sum_s)

    for n in range(0, heads, 2):
        at = slice(n * HEAD, (n + 2) * HEAD)
        do = _mm(by_h, wo_ref[at, :], 1, 1).astype(BF16)
        do_ref[:, at] = do
        o = o_ref[:, at]
        both = do.astype(F32) * o.astype(F32)
        for m in range(2):
            delta_ref[n + m : n + m + 1, :] = both[:, m * HEAD : (m + 1) * HEAD].T.sum(axis=0, keepdims=True)
        sum_s[at, :] += _mm(o.T, by_h)

    @pl.when(pl.program_id(0) == pl.num_programs(0) - 1)
    def _():
        by_w_ref[...] = sum_s[...].astype(BF16)


def out_back(by_h, wo, o):
    t, d = by_h.shape
    wide = o.shape[1]
    bt = _fit(t, 512)
    rows = lambda i: (i, 0)
    return _call(
        _out_back, (t // bt,),
        [(by_h, (bt, d), rows), (wo, None), (o, (bt, wide), rows)],
        [((t, wide), BF16, (bt, wide), rows), ((wide // HEAD, t), F32, (wide // HEAD, bt), lambda i: (0, i)), (wo.shape, BF16, wo.shape, lambda i: (0, 0))],
        [pltpu.VMEM(wo.shape, F32)], 4 * t * wo.size,
    )


def _attend_back(q_ref, k_ref, v_ref, do_ref, lse_ref, delta_ref, cos_ref, sin_ref, dq_ref, dk_ref, dv_ref, dq_s, dk_s, dv_s, *, bk, wide):
    g, bq, d = q_ref.shape
    cols = g * bq
    iq = pl.program_id(0)
    scale = d**-0.5
    e = scale * LOG2E
    per = wide // bq
    pieces = range(0, cols, wide)

    @pl.when(iq == 0)
    def _():
        dk_s[...] = jnp.zeros_like(dk_s)
        dv_s[...] = jnp.zeros_like(dv_s)

    dq_s[...] = jnp.zeros_like(dq_s)
    lses = jnp.concatenate([lse_ref[n : n + 1, :] for n in range(g)], axis=1) * LOG2E
    deltas = jnp.concatenate([delta_ref[n : n + 1, :] for n in range(g)], axis=1)

    def block(at_key, size, masked):
        here = pl.ds(pl.multiple_of(at_key, bq), size)
        keys, values = k_ref[here, :], v_ref[here, :]
        turned = keys.T
        qs = [q_ref[...].reshape(cols, d)[at : at + wide, :] for at in pieces]
        dos = [jnp.concatenate([do_ref[:, (n + at // bq) * d : (n + at // bq + 1) * d] for n in range(per)], axis=0) for at in pieces]
        scores = [_mm(keys, x, 1, 1) for x in qs]
        dps = [_mm(values, x, 1, 1) for x in dos]
        ok = _level(size, wide, bq) if masked else None
        for n, at in enumerate(pieces):
            p = jnp.exp2(scores[n] * e - lses[:, at : at + wide])
            if masked:
                p = jnp.where(ok, p, 0.0)
            ds = (p * (dps[n] - deltas[:, at : at + wide])).astype(BF16)
            dv_s[here, :] += _mm(p.astype(BF16), dos[n])
            dk_s[here, :] += _mm(ds, qs[n])
            dq_s[:, at : at + wide] += _mm(turned, ds)

    _spans(iq, bq, bk, block)
    cos, sin = cos_ref[...], -sin_ref[...]
    for n in range(g):
        dq_ref[:, n * d : (n + 1) * d] = _turned((dq_s[:, n * bq : (n + 1) * bq] * scale).T, cos, sin)

    @pl.when(iq == pl.num_programs(0) - 1)
    def _():
        dk_ref[...] = (dk_s[...] * scale).astype(BF16)
        dv_ref[...] = dv_s[...].astype(BF16)


def attend_back(q, k, v, do, lse, delta, cos, sin, beside):
    g, t, d = q.shape
    bq = _fit(t, 128)
    bk = _fit(t, 512)
    wide = _fit(g * bq, 512, bq)
    rows = lambda i: (i, 0)
    stats = ((g, bq), lambda i: (0, i))
    return _call(
        functools.partial(_attend_back, bk=bk, wide=wide), (t // bq,),
        [(q, (g, bq, d), lambda i: (0, i, 0)), (k, None), (v, None), (do, (bq, g * d), rows), (lse, *stats), (delta, *stats),
         (cos, (bq, d), rows), (sin, (bq, d), rows)],
        [((t, g * d), BF16, (bq, g * d), rows), (k.shape, BF16, k.shape, lambda i: (0, 0)), (v.shape, BF16, v.shape, lambda i: (0, 0))],
        [pltpu.VMEM((d, g * bq), F32), pltpu.VMEM(k.shape, F32), pltpu.VMEM(v.shape, F32)],
        5 * g * t * t * d, g * t * t // 2, beside,
    )


def _qkv_back(h_ref, by_h_ref, dq_ref, dk_ref, dv_ref, cos_ref, sin_ref, w_ref, out_ref, by_w_ref, sum_s):
    wide, scale, a = _normed(h_ref[...])
    at = a.T

    @pl.when(pl.program_id(0) == 0)
    def _():
        sum_s[...] = jnp.zeros_like(sum_s)

    heads = dq_ref.shape[1] // HEAD
    rest = jnp.concatenate([_turned(dk_ref[...], cos_ref[...], -sin_ref[...]), dv_ref[...]], axis=1)
    by_a = jnp.zeros(wide.shape, F32)
    for n in range(0, heads + 2, 2):
        here = slice(n * HEAD, (n + 2) * HEAD)
        g = dq_ref[:, here] if n < heads else rest
        by_a = by_a + _mm(g, w_ref[:, here], 1, 1)
        sum_s[:, here] += _mm(at, g)
    out_ref[...] = _plus(by_h_ref[...], _norm_back(wide, scale, by_a))

    @pl.when(pl.program_id(0) == pl.num_programs(0) - 1)
    def _():
        by_w_ref[...] = sum_s[...].astype(BF16)


def qkv_back(h, by_h, dq, dk, dv, cos, sin, w):
    t, d = h.shape
    bt = _fit(t, 512)
    rows = lambda i: (i, 0)
    tile = lambda a: (a, (bt, a.shape[1]), rows)
    return _call(
        _qkv_back, (t // bt,),
        [*(tile(a) for a in (h, by_h, dq, dk, dv, cos, sin)), (w, None)],
        [(h.shape, BF16, (bt, d), rows), (w.shape, BF16, w.shape, lambda i: (0, 0))],
        [pltpu.VMEM(w.shape, F32)], 4 * t * w.size,
    )


def _mlp(h_ref, o_ref, wo_ref, gu_ref, down_ref, h2_ref, y_ref, *, chunk):
    h2 = _plus(h_ref[...], _mm(o_ref[...], wo_ref[...]))
    h2_ref[...] = h2
    b = _normed(h2)[2]
    ff = down_ref.shape[0]
    y = jnp.zeros(h_ref.shape, F32)
    for c in range(0, ff, chunk):
        gate = _mm(b, gu_ref[:, c : c + chunk])
        up = _mm(b, gu_ref[:, ff + c : ff + c + chunk])
        y = y + _mm((gate * jax.nn.sigmoid(gate) * up).astype(BF16), down_ref[c : c + chunk, :])
    y_ref[...] = _plus(h2, y)


def mlp(h, o, wo, gu, down, beside):
    t, d = h.shape
    bt = _fit(t, 512)
    rows = lambda i: (i, 0)
    return _call(
        functools.partial(_mlp, chunk=_fit(down.shape[0], 512)), (t // bt,),
        [(h, (bt, d), rows), (o, (bt, o.shape[1]), rows), (wo, None), (gu, None), (down, None)], [(h.shape, BF16, (bt, d), rows)] * 2, [],
        2 * t * (wo.size + gu.size + down.size), t * down.shape[0], beside,
    )


def _mlp_back(*refs, chunk, project):
    if project:
        o_ref, wo_ref, *refs = refs
    h_ref, dy_ref, gu_ref, down_ref, out_ref, by_gu_ref, by_down_ref, gu_s, down_s = refs
    wide, scale, b = _normed(_plus(h_ref[...], _mm(o_ref[...], wo_ref[...])) if project else h_ref[...])
    bt = b.T
    dy = dy_ref[...]
    ff = down_ref.shape[0]

    @pl.when(pl.program_id(0) == 0)
    def _():
        gu_s[...] = jnp.zeros_like(gu_s)
        down_s[...] = jnp.zeros_like(down_s)

    by_b = jnp.zeros(wide.shape, F32)
    for c in range(0, ff, chunk):
        g, u = slice(c, c + chunk), slice(ff + c, ff + c + chunk)
        gate, up = _mm(b, gu_ref[:, g]), _mm(b, gu_ref[:, u])
        by = _mm(dy, down_ref[g, :], 1, 1).astype(BF16).astype(F32)
        part = jax.nn.sigmoid(gate)
        silu = gate * part
        by_up = (by * silu).astype(BF16)
        by_gate = (by * up * (part * (1 + gate * (1 - part)))).astype(BF16)
        down_s[g, :] += _mm((silu * up).astype(BF16).T, dy)
        by_b = by_b + _mm(by_gate, gu_ref[:, g], 1, 1) + _mm(by_up, gu_ref[:, u], 1, 1)
        gu_s[:, g] += _mm(bt, by_gate)
        gu_s[:, u] += _mm(bt, by_up)
    out_ref[...] = _plus(dy, _norm_back(wide, scale, by_b))

    @pl.when(pl.program_id(0) == pl.num_programs(0) - 1)
    def _():
        by_gu_ref[...] = gu_s[...].astype(BF16)
        by_down_ref[...] = down_s[...].astype(BF16)


def mlp_back(h, dy, gu, down, beside, o=None, wo=None):
    t, d = h.shape
    bt = _fit(t, 512)
    rows = lambda i: (i, 0)
    return _call(
        functools.partial(_mlp_back, chunk=_fit(down.shape[0], 256), project=o is not None), (t // bt,),
        ([] if o is None else [(o, (bt, o.shape[1]), rows), (wo, None)]) + [(h, (bt, d), rows), (dy, (bt, d), rows), (gu, None), (down, None)],
        [(h.shape, BF16, (bt, d), rows), (gu.shape, BF16, gu.shape, lambda i: (0, 0)), (down.shape, BF16, down.shape, lambda i: (0, 0))],
        [pltpu.VMEM(gu.shape, F32), pltpu.VMEM(down.shape, F32)], 6 * t * (gu.size + down.size), t * down.shape[0], beside,
    )


def tables(t, head):
    half = head // 2
    angle = jnp.arange(t, dtype=F32)[:, None] * THETA ** (-jnp.arange(half, dtype=F32) / half)
    cos, sin = jnp.cos(angle), jnp.sin(angle)
    return jnp.concatenate([cos, cos], 1), jnp.concatenate([-sin, sin], 1)


def adamw(w, m, v, g):
    m = 0.9 * m + 0.1 * g
    v = 0.95 * v + 0.05 * g * g
    step = m * lax.rsqrt(v + 1e-8) + 0.1 * w
    return (w - 0.02 * step).astype(BF16), m, v


def clipped(gradients, sum_of_squares, count):
    factor = jnp.minimum(1.0, 0.5 * lax.rsqrt(sum_of_squares / count + 1e-30))
    return [g * factor for g in gradients]


def solution(mesh):
    def step(x, dy, *arrays):
        weights, m, v = (arrays[i : i + 7] for i in (0, 7, 14))
        layers = weights[0].shape[0]
        wq, wk, wv, wo, w_gate, w_up, w_down = weights
        ids = itertools.count()
        qkv_of = lambda n: jnp.concatenate([wq[n], wk[n], wv[n]], axis=1)
        h = x[0]
        cos, sin = tables(h.shape[0], HEAD)
        kept = []
        (w_qkv,) = alone(Gather(next(ids), [qkv_of(0)], [-1]))
        for n in range(layers):
            q, k, val = qkv(h, w_qkv, cos, sin)
            fetch = Gather(next(ids), [wo[n], jnp.concatenate([w_gate[n], w_up[n]], axis=1), w_down[n]], [5, 7, -1])
            o, lse, w_o, w_gu, w_d = attend(q, k, val, fetch)
            kept.append([h, q, k, val, o, lse, None, w_qkv, w_o, w_gu, w_d])
            if n < layers - 1:
                h2, h, w_qkv = mlp(h, o, w_o, w_gu, w_d, Gather(next(ids), [qkv_of(n + 1)], [3]))
                kept[n][6] = h2

        me, devices = lax.axis_index("dp"), lax.axis_size("dp")

        def total(term, come):
            size = term.shape[0] // devices
            parts = [lax.dynamic_slice_in_dim(term, me * size, size, 0), *(come[i] for i in range(devices - 1))]
            return sum(p.astype(F32) for p in parts).astype(BF16)

        by_h, mine, left = dy[0], [[None] * 4 for _ in range(layers)], []
        for n in reversed(range(layers)):
            h, q, k, val, o, lse, h2, w_qkv, w_o, w_gu, w_d = kept[n]
            last = n == layers - 1
            beside = Scatter(next(ids), left) if left else None
            by_h, by_gu, by_d, *come = mlp_back(h if last else h2, by_h, w_gu, w_d, beside, *((o, w_o) if last else ()))
            if left:
                mine[n + 1][:2] = [total(t, c) for t, c in zip(left, come, strict=True)]
            do, delta, by_o = out_back(by_h, w_o, o)
            terms = [by_gu, by_d] + ([by_o] if n == 0 else [])
            dq, dk, dv, *come = attend_back(q, k, val, do, lse, delta, cos, sin, Scatter(next(ids), terms))
            sums = [total(t, c) for t, c in zip(terms, come, strict=True)]
            mine[n][2:] = sums[:2]
            by_h, by_qkv = qkv_back(h, by_h, dq, dk, dv, cos, sin, w_qkv)
            left = [by_qkv, by_o]
            if n == 0:
                mine[n][1] = sums[2]
                mine[n][0] = total(by_qkv, alone(Scatter(next(ids), [by_qkv]))[0])
        e, f, ff = wq.shape[2], wq.shape[2] + wk.shape[2], w_gate.shape[2]
        mine = [[a[:, :e], a[:, e:f], a[:, f:], b, c[:, :ff], c[:, ff:], d] for a, b, c, d in mine]
        gradients = [jnp.stack([mine[n][i] for n in range(layers)]).astype(F32) for i in range(7)]
        squares = lax.psum(sum(jnp.sum(g * g) for g in gradients), "dp")
        gradients = clipped(gradients, squares, lax.psum(1, "dp") * sum(g.size for g in gradients))
        new = [adamw(w.astype(F32), m, v, g) for w, m, v, g in zip(weights, m, v, gradients, strict=True)]
        return tuple(one[which] for which in range(3) for one in new)

    states, cut = P(("rep", "dp"), None, None), P(None, "dp", None)
    return jax.shard_map(
        step,
        mesh=mesh,
        in_specs=(states, states) + (cut,) * 21,
        out_specs=(P("rep", "dp", None),) * 21,
        check_vma=False,
    )
```

```python
import functools
import itertools

import jax
import jax.numpy as jnp
import numpy as np
from jax import lax
from jax.experimental import pallas as pl
from jax.experimental.pallas import tpu as pltpu
from jax.sharding import PartitionSpec as P

HEAD = 128
THETA = 10000
NAMES = ("wq", "wk", "wv", "wo", "w_gate", "w_up", "w_down")
NEG = -1e30
HIDDEN = 2 * NEG
LOG2E = 1.4426950408889634
VMEM = 60 * 2**20
F32, BF16 = jnp.float32, jnp.bfloat16


def _mm(a, b, ca=1, cb=0):
    return lax.dot_general(a, b, (((ca,), (cb,)), ((), ())), preferred_element_type=F32)


def _fit(size, want, unit=128):
    return max(n for n in range(unit, max(min(want, size), unit) + 1, unit) if size % n == 0)


def _normed(h):
    wide = h.astype(F32)
    scale = lax.rsqrt(jnp.mean(wide * wide, -1, keepdims=True) + 1e-6)
    return wide, scale, (wide * scale).astype(BF16)


def _norm_back(wide, scale, by_a):
    by_a = by_a.astype(BF16).astype(F32)
    along = jnp.sum(by_a * wide, -1, keepdims=True) * (scale * scale * scale) * (1 / wide.shape[-1])
    return (by_a * scale - wide * along).astype(BF16)


def _plus(a, b):
    return (a.astype(F32) + b.astype(BF16).astype(F32)).astype(BF16)


def _turned(t, cos, sin):
    t = t.astype(BF16).astype(F32)
    return (t * cos + pltpu.roll(t, t.shape[1] // 2, 1) * sin).astype(BF16)


MESH = pl.DeviceIdType.MESH


class Gather:
    def __init__(self, number, pieces):
        self.number, self.pieces = number, pieces
        self.arrays = [p[0] for p in pieces]

    def ins(self):
        def block(n):
            return lambda *_: (n, 0, 0)

        return [(p[0], (1, *p[0].shape[1:]), block(p[1]), pl.Buffered(1)) for p in self.pieces]

    def outs(self, n):
        wholes = {}
        for a, _, _, width, whole, _, _ in self.pieces:
            wholes[whole] = (n * a.shape[1], wholes.get(whole, (0, 0))[1] + width)
        return [wholes[i] for i in range(len(wholes))]

    def scratch(self):
        return [pltpu.SemaphoreType.DMA((len(self.pieces), 3))] * 4 + [pltpu.SemaphoreType.DMA((len(self.pieces),))]

    def run(self, step, last, shards, wholes, scratch, before):
        send, come, give, get, own = scratch
        me, rep, n = lax.axis_index("dp"), lax.axis_index("rep"), lax.axis_size("dp")
        core = lax.rem(rep, 2)
        partner = rep + 1 - 2 * core
        place = [(wholes[p[4]], pl.ds(p[2], p[3]), pl.ds(p[5], p[3]), p[0].shape[1] // 2) for p in self.pieces]

        def rows(half, owner, which):
            return pl.ds(pl.multiple_of((2 * owner + which) * half, half), half)

        def out(i, d):
            whole, cols, at, half = place[i]
            return pltpu.make_async_remote_copy(
                src_ref=shards[i].at[0, rows(half, 0, core), cols], dst_ref=whole.at[rows(half, me, core), at],
                send_sem=send.at[i, d - 1], recv_sem=come.at[i, d - 1], device_id={"dp": lax.rem(me + d, n)}, device_id_type=MESH)

        def over(i, d):
            whole, _, at, half = place[i]
            where = rows(half, lax.rem(me + n - d, n), core)
            return pltpu.make_async_remote_copy(
                src_ref=whole.at[where, at], dst_ref=whole.at[where, at],
                send_sem=give.at[i, d - 1], recv_sem=get.at[i, d - 1], device_id={"rep": partner}, device_id_type=MESH)

        def mine(i):
            whole, cols, at, half = place[i]
            return pltpu.make_async_copy(shards[i].at[0, :, cols], whole.at[pl.ds(pl.multiple_of(me * 2 * half, 2 * half), 2 * half), at], own.at[i])

        count = len(self.pieces)
        all_ = [(i, d) for i in range(count) for d in range(1, n)]
        if before:

            @pl.when(step == 0)
            def _():
                barrier = pltpu.get_barrier_semaphore()
                for d in range(1, n):
                    pl.semaphore_signal(barrier, inc=1, device_id={"dp": lax.rem(me + d, n)}, device_id_type=MESH)
                pl.semaphore_signal(barrier, inc=1, device_id={"rep": partner}, device_id_type=MESH)
                pl.semaphore_wait(barrier, n)
                for i, d in all_:
                    out(i, d).start()
                for i in range(count):
                    mine(i).start()

        for when in sorted({p[6] for p in self.pieces}):
            if before == (when >= 0):

                @pl.when(step == (when if when >= 0 else last))
                def _():
                    for i, d in all_:
                        if self.pieces[i][6] == when:
                            out(i, d).wait_recv()
                            over(i, d).start()

        if not before:

            @pl.when(step == last)
            def _():
                for i, d in all_:
                    out(i, d).wait_send()
                    over(i, d).wait()
                for i in range(count):
                    mine(i).wait()


class Scatter:
    def __init__(self, number, arrays):
        self.number, self.arrays = number, arrays

    def ins(self):
        return [(a, pltpu.HBM) for a in self.arrays]

    def outs(self, n):
        return [(n - 1, a.shape[0] // n, a.shape[1]) for a in self.arrays]

    def scratch(self):
        return [pltpu.SemaphoreType.DMA((len(self.arrays), 3))] * 2

    def run(self, step, last, terms, comes, scratch, before):
        send, come = scratch
        me, n = lax.axis_index("dp"), lax.axis_size("dp")

        def out(i, d):
            to = lax.rem(me + d, n)
            size = terms[i].shape[0] // n
            return pltpu.make_async_remote_copy(
                src_ref=terms[i].at[pl.ds(pl.multiple_of(to * size, size), size), :], dst_ref=comes[i].at[d - 1],
                send_sem=send.at[i, d - 1], recv_sem=come.at[i, d - 1], device_id={"dp": to}, device_id_type=MESH)

        all_ = [(i, d) for i in range(len(terms)) for d in range(1, n)]

        if before:

            @pl.when(step == 0)
            def _():
                barrier = pltpu.get_barrier_semaphore()
                for d in range(1, n):
                    pl.semaphore_signal(barrier, inc=1, device_id={"dp": lax.rem(me + d, n)}, device_id_type=MESH)
                pl.semaphore_wait(barrier, n - 1)
                for i, d in all_:
                    out(i, d).start()

        else:

            @pl.when(step == last)
            def _():
                for i, d in all_:
                    out(i, d).wait()


def _call(kernel, grid, ins, outs, scratch, flops, exp=0, beside=None):
    whole = lambda a: pl.BlockSpec(a.shape, lambda *_: (0,) * a.ndim, pipeline_mode=pl.Buffered(1))
    spec = lambda i: whole(i[0]) if i[1] is None else pl.BlockSpec(memory_space=i[1]) if i[1] is pltpu.HBM else pl.BlockSpec(i[1], i[2], pipeline_mode=i[3] if len(i) > 3 else None)
    size = sum(i[0].size * i[0].dtype.itemsize for i in ins)
    out_specs = [pl.BlockSpec(o[2], o[3]) for o in outs]
    shapes = [jax.ShapeDtypeStruct(o[0], o[1]) for o in outs]
    body, more = kernel, {}
    if beside is not None:
        more = dict(collective_id=beside.number, has_side_effects=True)
        wholes = beside.outs(lax.axis_size("dp"))
        counts = [len(ins), len(beside.arrays), len(outs), len(wholes), len(scratch)]
        ins = ins + beside.ins()
        shapes += [jax.ShapeDtypeStruct(o, BF16) for o in wholes]
        out_specs += [pl.BlockSpec(memory_space=pltpu.HBM)] * len(wholes)
        scratch = scratch + beside.scratch()

        def body(*refs):
            split, at = [], 0
            for c in counts:
                split.append(refs[at : at + c])
                at += c
            step, last = pl.program_id(0), pl.num_programs(0) - 1
            beside.run(step, last, split[1], split[3], refs[at:], True)
            kernel(*split[0], *split[2], *split[4])
            beside.run(step, last, split[1], split[3], refs[at:], False)

    return pl.pallas_call(
        body,
        grid=grid,
        in_specs=[spec(i) for i in ins],
        out_specs=out_specs,
        out_shape=shapes,
        scratch_shapes=scratch,
        compiler_params=pltpu.CompilerParams(dimension_semantics=("arbitrary",) * len(grid), vmem_limit_bytes=VMEM, **more),
        cost_estimate=pl.CostEstimate(flops=flops, transcendentals=exp, bytes_accessed=2 * size),
    )(*[i[0] for i in ins])


def alone(beside):
    return _call(lambda: None, (1,), [], [], [], 0, beside=beside)


def _qkv(h_ref, w_ref, cos_ref, sin_ref, q_ref, k_ref, v_ref):
    a = _normed(h_ref[...])[2]
    cos, sin = cos_ref[...], sin_ref[...]
    heads = q_ref.shape[0]
    for n in range(0, heads + 2, 2):
        y = _mm(a, w_ref[:, n * HEAD : (n + 2) * HEAD])
        for at in range(n, n + 2):
            part = y[:, (at - n) * HEAD : (at - n + 1) * HEAD]
            if at < heads:
                q_ref[at] = _turned(part, cos, sin)
            elif at == heads:
                k_ref[...] = _turned(part, cos, sin)
            else:
                v_ref[...] = part.astype(BF16)


def qkv(h, w, cos, sin):
    t, d = h.shape
    heads = w.shape[1] // HEAD - 2
    bt = _fit(t, 512)
    rows = lambda i: (i, 0)
    return _call(
        _qkv, (t // bt,),
        [(h, (bt, d), rows), (w, None), (cos, (bt, HEAD), rows), (sin, (bt, HEAD), rows)],
        [((heads, t, HEAD), BF16, (heads, bt, HEAD), lambda i: (0, i, 0)), ((t, HEAD), BF16, (bt, HEAD), rows), ((t, HEAD), BF16, (bt, HEAD), rows)],
        [], 2 * t * d * w.shape[1],
    )


def _spans(iq, bq, bk, block):
    lax.fori_loop(0, lax.div(iq * bq, bk), lambda j, _: block(j * bk, bk, False), None)
    rest = lax.rem(iq, bk // bq)
    for n in range(bk // bq):

        @pl.when(rest == n)
        def _():
            block((iq - n) * bq, (n + 1) * bq, True)


def _level(size, wide, bq):
    return (lax.broadcasted_iota(jnp.int32, (size, wide), 0) - lax.rem(lax.broadcasted_iota(jnp.int32, (size, wide), 1), bq)) <= size - bq


def _attend(q_ref, k_ref, v_ref, o_ref, lse_ref, top_s, mix_s, *, bk, wide):
    g, bq, d = q_ref.shape
    cols = g * bq
    iq = pl.program_id(0)
    scale = d**-0.5
    e = scale * LOG2E
    pieces = range(0, cols, wide)
    top_s[...] = jnp.full((1, cols), NEG, F32)
    mix_s[...] = jnp.zeros((d + 8, cols), F32)

    def block(at_key, size, masked):
        here = pl.ds(pl.multiple_of(at_key, bq), size)
        keys = k_ref[here, :]
        values = jnp.concatenate([v_ref[here, :].T, jnp.ones((8, size), BF16)], axis=0)
        scores = [_mm(keys, q_ref[...].reshape(cols, d)[at : at + wide, :], 1, 1) for at in pieces]
        ok = _level(size, wide, bq) if masked else None
        weights, keeps = [], []
        for at, s in zip(pieces, scores):
            if masked:
                s = jnp.where(ok, s, HIDDEN)
            old = top_s[:, at : at + wide]
            top = jnp.maximum(old, s.max(axis=0, keepdims=True))
            top_s[:, at : at + wide] = top
            weights.append(jnp.exp2((s - top) * e).astype(BF16))
            keeps.append(jnp.exp2((old - top) * e))
        for at, p, keep in zip(pieces, weights, keeps):
            mix_s[:, at : at + wide] = mix_s[:, at : at + wide] * keep + _mm(values, p)

    _spans(iq, bq, bk, block)
    for n in range(g):
        at = slice(n * bq, (n + 1) * bq)
        total = mix_s[d : d + 1, at]
        o_ref[:, n * d : (n + 1) * d] = (mix_s[:d, at] * (1 / total)).T.astype(BF16)
        lse_ref[n : n + 1, :] = top_s[:, at] * scale + jnp.log(total)


def attend(q, k, v, beside):
    g, t, d = q.shape
    bq = _fit(t, 256)
    bk = _fit(t, 512)
    wide = _fit(g * bq, 512, bq)
    rows = lambda i: (i, 0)
    return _call(
        functools.partial(_attend, bk=bk, wide=wide), (t // bq,),
        [(q, (g, bq, d), lambda i: (0, i, 0)), (k, None), (v, None)],
        [((t, g * d), BF16, (bq, g * d), rows), ((g, t), F32, (g, bq), lambda i: (0, i))],
        [pltpu.VMEM((1, g * bq), F32), pltpu.VMEM((d + 8, g * bq), F32)],
        2 * g * t * t * d, g * t * t // 2, beside,
    )


def _out_back(by_h_ref, wo_ref, o_ref, do_ref, delta_ref, by_w_ref, sum_s):
    by_h = by_h_ref[...]
    heads = o_ref.shape[1] // HEAD

    @pl.when(pl.program_id(0) == 0)
    def _():
        sum_s[...] = jnp.zeros_like(sum_s)

    for n in range(0, heads, 2):
        at = slice(n * HEAD, (n + 2) * HEAD)
        do = _mm(by_h, wo_ref[at, :], 1, 1).astype(BF16)
        do_ref[:, at] = do
        o = o_ref[:, at]
        both = do.astype(F32) * o.astype(F32)
        for m in range(2):
            delta_ref[n + m : n + m + 1, :] = both[:, m * HEAD : (m + 1) * HEAD].T.sum(axis=0, keepdims=True)
        sum_s[at, :] += _mm(o.T, by_h)

    @pl.when(pl.program_id(0) == pl.num_programs(0) - 1)
    def _():
        by_w_ref[...] = sum_s[...].astype(BF16)


def out_back(by_h, wo, o):
    t, d = by_h.shape
    wide = o.shape[1]
    bt = _fit(t, 512)
    rows = lambda i: (i, 0)
    return _call(
        _out_back, (t // bt,),
        [(by_h, (bt, d), rows), (wo, None), (o, (bt, wide), rows)],
        [((t, wide), BF16, (bt, wide), rows), ((wide // HEAD, t), F32, (wide // HEAD, bt), lambda i: (0, i)), (wo.shape, BF16, wo.shape, lambda i: (0, 0))],
        [pltpu.VMEM(wo.shape, F32)], 4 * t * wo.size,
    )


def _attend_back(q_ref, k_ref, v_ref, do_ref, lse_ref, delta_ref, cos_ref, sin_ref, dq_ref, dk_ref, dv_ref, dq_s, dk_s, dv_s, *, bk, wide):
    g, bq, d = q_ref.shape
    cols = g * bq
    iq = pl.program_id(0)
    scale = d**-0.5
    e = scale * LOG2E
    per = wide // bq
    pieces = range(0, cols, wide)

    @pl.when(iq == 0)
    def _():
        dk_s[...] = jnp.zeros_like(dk_s)
        dv_s[...] = jnp.zeros_like(dv_s)

    dq_s[...] = jnp.zeros_like(dq_s)
    lses = jnp.concatenate([lse_ref[n : n + 1, :] for n in range(g)], axis=1) * LOG2E
    deltas = jnp.concatenate([delta_ref[n : n + 1, :] for n in range(g)], axis=1)

    def block(at_key, size, masked):
        here = pl.ds(pl.multiple_of(at_key, bq), size)
        keys, values = k_ref[here, :], v_ref[here, :]
        turned = keys.T
        qs = [q_ref[...].reshape(cols, d)[at : at + wide, :] for at in pieces]
        dos = [jnp.concatenate([do_ref[:, (n + at // bq) * d : (n + at // bq + 1) * d] for n in range(per)], axis=0) for at in pieces]
        scores = [_mm(keys, x, 1, 1) for x in qs]
        dps = [_mm(values, x, 1, 1) for x in dos]
        ok = _level(size, wide, bq) if masked else None
        for n, at in enumerate(pieces):
            p = jnp.exp2(scores[n] * e - lses[:, at : at + wide])
            if masked:
                p = jnp.where(ok, p, 0.0)
            ds = (p * (dps[n] - deltas[:, at : at + wide])).astype(BF16)
            dv_s[here, :] += _mm(p.astype(BF16), dos[n])
            dk_s[here, :] += _mm(ds, qs[n])
            dq_s[:, at : at + wide] += _mm(turned, ds)

    _spans(iq, bq, bk, block)
    cos, sin = cos_ref[...], -sin_ref[...]
    for n in range(g):
        dq_ref[:, n * d : (n + 1) * d] = _turned((dq_s[:, n * bq : (n + 1) * bq] * scale).T, cos, sin)

    @pl.when(iq == pl.num_programs(0) - 1)
    def _():
        dk_ref[...] = (dk_s[...] * scale).astype(BF16)
        dv_ref[...] = dv_s[...].astype(BF16)


def attend_back(q, k, v, do, lse, delta, cos, sin, beside):
    g, t, d = q.shape
    bq = _fit(t, 128)
    bk = _fit(t, 512)
    wide = _fit(g * bq, 512, bq)
    rows = lambda i: (i, 0)
    stats = ((g, bq), lambda i: (0, i))
    return _call(
        functools.partial(_attend_back, bk=bk, wide=wide), (t // bq,),
        [(q, (g, bq, d), lambda i: (0, i, 0)), (k, None), (v, None), (do, (bq, g * d), rows), (lse, *stats), (delta, *stats),
         (cos, (bq, d), rows), (sin, (bq, d), rows)],
        [((t, g * d), BF16, (bq, g * d), rows), (k.shape, BF16, k.shape, lambda i: (0, 0)), (v.shape, BF16, v.shape, lambda i: (0, 0))],
        [pltpu.VMEM((d, g * bq), F32), pltpu.VMEM(k.shape, F32), pltpu.VMEM(v.shape, F32)],
        5 * g * t * t * d, g * t * t // 2, beside,
    )


def _qkv_back(h_ref, by_h_ref, dq_ref, dk_ref, dv_ref, cos_ref, sin_ref, w_ref, out_ref, by_w_ref, sum_s):
    wide, scale, a = _normed(h_ref[...])
    at = a.T

    @pl.when(pl.program_id(0) == 0)
    def _():
        sum_s[...] = jnp.zeros_like(sum_s)

    heads = dq_ref.shape[1] // HEAD
    rest = jnp.concatenate([_turned(dk_ref[...], cos_ref[...], -sin_ref[...]), dv_ref[...]], axis=1)
    by_a = jnp.zeros(wide.shape, F32)
    for n in range(0, heads + 2, 2):
        here = slice(n * HEAD, (n + 2) * HEAD)
        g = dq_ref[:, here] if n < heads else rest
        by_a = by_a + _mm(g, w_ref[:, here], 1, 1)
        sum_s[:, here] += _mm(at, g)
    out_ref[...] = _plus(by_h_ref[...], _norm_back(wide, scale, by_a))

    @pl.when(pl.program_id(0) == pl.num_programs(0) - 1)
    def _():
        by_w_ref[...] = sum_s[...].astype(BF16)


def qkv_back(h, by_h, dq, dk, dv, cos, sin, w):
    t, d = h.shape
    bt = _fit(t, 512)
    rows = lambda i: (i, 0)
    tile = lambda a: (a, (bt, a.shape[1]), rows)
    return _call(
        _qkv_back, (t // bt,),
        [*(tile(a) for a in (h, by_h, dq, dk, dv, cos, sin)), (w, None)],
        [(h.shape, BF16, (bt, d), rows), (w.shape, BF16, w.shape, lambda i: (0, 0))],
        [pltpu.VMEM(w.shape, F32)], 4 * t * w.size,
    )


def _mlp(h_ref, o_ref, wo_ref, gu_ref, down_ref, h2_ref, y_ref, *, chunk):
    h2 = _plus(h_ref[...], _mm(o_ref[...], wo_ref[...]))
    h2_ref[...] = h2
    b = _normed(h2)[2]
    ff = down_ref.shape[0]
    y = jnp.zeros(h_ref.shape, F32)
    for c in range(0, ff, chunk):
        gate = _mm(b, gu_ref[:, c : c + chunk])
        up = _mm(b, gu_ref[:, ff + c : ff + c + chunk])
        y = y + _mm((gate * jax.nn.sigmoid(gate) * up).astype(BF16), down_ref[c : c + chunk, :])
    y_ref[...] = _plus(h2, y)


def mlp(h, o, wo, gu, down, beside):
    t, d = h.shape
    bt = _fit(t, 512)
    rows = lambda i: (i, 0)
    return _call(
        functools.partial(_mlp, chunk=_fit(down.shape[0], 512)), (t // bt,),
        [(h, (bt, d), rows), (o, (bt, o.shape[1]), rows), (wo, None), (gu, None), (down, None)], [(h.shape, BF16, (bt, d), rows)] * 2, [],
        2 * t * (wo.size + gu.size + down.size), t * down.shape[0], beside,
    )


def _mlp_back(*refs, chunk, project):
    if project:
        o_ref, wo_ref, *refs = refs
    h_ref, dy_ref, gu_ref, down_ref, out_ref, by_gate_ref, by_up_ref, by_down_ref, gu_s, down_s = refs
    wide, scale, b = _normed(_plus(h_ref[...], _mm(o_ref[...], wo_ref[...])) if project else h_ref[...])
    bt = b.T
    dy = dy_ref[...]
    ff = down_ref.shape[0]

    @pl.when(pl.program_id(0) == 0)
    def _():
        gu_s[...] = jnp.zeros_like(gu_s)
        down_s[...] = jnp.zeros_like(down_s)

    by_b = jnp.zeros(wide.shape, F32)
    for c in range(0, ff, chunk):
        g, u = slice(c, c + chunk), slice(ff + c, ff + c + chunk)
        gate, up = _mm(b, gu_ref[:, g]), _mm(b, gu_ref[:, u])
        by = _mm(dy, down_ref[g, :], 1, 1).astype(BF16).astype(F32)
        part = jax.nn.sigmoid(gate)
        silu = gate * part
        by_up = (by * silu).astype(BF16)
        by_gate = (by * up * (part * (1 + gate * (1 - part)))).astype(BF16)
        down_s[g, :] += _mm((silu * up).astype(BF16).T, dy)
        by_b = by_b + _mm(by_gate, gu_ref[:, g], 1, 1) + _mm(by_up, gu_ref[:, u], 1, 1)
        gu_s[:, g] += _mm(bt, by_gate)
        gu_s[:, u] += _mm(bt, by_up)
    out_ref[...] = _plus(dy, _norm_back(wide, scale, by_b))

    @pl.when(pl.program_id(0) == pl.num_programs(0) - 1)
    def _():
        by_gate_ref[...] = gu_s[:, :ff].astype(BF16)
        by_up_ref[...] = gu_s[:, ff:].astype(BF16)
        by_down_ref[...] = down_s[...].astype(BF16)


def mlp_back(h, dy, gu, down, beside, o=None, wo=None):
    t, d = h.shape
    bt = _fit(t, 512)
    rows = lambda i: (i, 0)
    return _call(
        functools.partial(_mlp_back, chunk=_fit(down.shape[0], 256), project=o is not None), (t // bt,),
        ([] if o is None else [(o, (bt, o.shape[1]), rows), (wo, None)]) + [(h, (bt, d), rows), (dy, (bt, d), rows), (gu, None), (down, None)],
        [(h.shape, BF16, (bt, d), rows), *[((d, down.shape[0]), BF16, (d, down.shape[0]), lambda i: (0, 0))] * 2, (down.shape, BF16, down.shape, lambda i: (0, 0))],
        [pltpu.VMEM(gu.shape, F32), pltpu.VMEM(down.shape, F32)], 6 * t * (gu.size + down.size), t * down.shape[0], beside,
    )


def tables(t, head):
    half = head // 2
    angle = np.arange(t, dtype=np.float32)[:, None] * (np.float32(THETA) ** (-np.arange(half, dtype=np.float32) / np.float32(half)))
    cos, sin = (f(angle.astype(np.float64)).astype(np.float32) for f in (np.cos, np.sin))
    return jnp.asarray(np.concatenate([cos, cos], 1)), jnp.asarray(np.concatenate([-sin, sin], 1))


def _finish(*refs, layers, count):
    terms, comes = refs[: layers * 5], refs[layers * 5 : layers * 10 - 1]
    outs, factor_ref = refs[layers * 10 - 1 : layers * 10 + 4], refs[layers * 10 + 4]
    own = refs[layers * 10 + 5 : layers * 15 + 5]
    come = refs[layers * 15 + 5 : layers * 20 + 5]
    squares_s, here_sem, come_sem, send, get, send_sum, get_sum = refs[layers * 20 + 5 :]
    me, n = lax.axis_index("dp"), lax.axis_size("dp")
    barrier = pltpu.get_barrier_semaphore()
    for d in range(1, n):
        pl.semaphore_signal(barrier, inc=1, device_id={"dp": lax.rem(me + d, n)}, device_id_type=MESH)
    pl.semaphore_wait(barrier, n - 1)

    def rows(i, owner):
        size = own[i].shape[0]
        return pl.ds(pl.multiple_of(owner * size, size), size)

    def out(d):
        to = lax.rem(me + d, n)
        return pltpu.make_async_remote_copy(src_ref=terms[0].at[rows(0, to), :], dst_ref=come[0].at[d - 1], send_sem=send.at[d - 1], recv_sem=get.at[d - 1],
                                            device_id={"dp": to}, device_id_type=MESH)

    for d in range(1, n):
        out(d).start()
    local = lambda i: pltpu.make_async_copy(terms[i].at[rows(i, me), :], own[i], here_sem.at[i])
    came = lambda i: pltpu.make_async_copy(comes[i - 1], come[i], come_sem.at[i])
    for i in [*range(1, layers * 5), 0]:
        local(i).start()
        if i:
            came(i).start()

    def total(i):
        size, columns = own[i].shape
        part = 16

        def some(j, squares):
            here = pl.ds(pl.multiple_of(j * part, part), part)
            g = own[i][here, :].astype(F32)
            for d in range(n - 1):
                g = g + come[i][d, here, :].astype(F32)
            g = g.astype(BF16)
            outs[i % 5][i // 5, here, :] = g
            g = g.astype(F32)
            g = g * g
            g = sum(g[:, c : c + HEAD] for c in range(0, columns, HEAD))
            return squares + g[:8] + g[8:]

        return lax.fori_loop(0, size // part, some, jnp.zeros((8, HEAD), F32))

    squares = jnp.zeros((8, HEAD), F32)
    for i in range(1, layers * 5):
        local(i).wait()
        came(i).wait()
        squares = squares + total(i)
    local(0).wait()
    for d in range(1, n):
        out(d).wait()
    squares_s[0] = squares + total(0)

    def tell(d):
        return pltpu.make_async_remote_copy(src_ref=squares_s.at[0], dst_ref=squares_s.at[d], send_sem=send_sum.at[d - 1], recv_sem=get_sum.at[d - 1],
                                            device_id={"dp": lax.rem(me + d, n)}, device_id_type=MESH)

    for d in range(1, n):
        tell(d).start()
    for d in range(1, n):
        tell(d).wait()
    all_ = jnp.zeros((8, HEAD), F32)
    for owner in range(n):
        all_ = all_ + squares_s[lax.rem(me + n - owner, n)]
    both = jnp.sum(jnp.sum(all_, axis=1, keepdims=True), axis=0, keepdims=True)
    factor_ref[...] = jnp.broadcast_to(jnp.minimum(1.0, 0.5 * lax.rsqrt(both / count + 1e-30)), factor_ref.shape)


def finish(number, terms, comes, layers):
    n = lax.axis_size("dp")
    mine = [(t.shape[0] // n, t.shape[1]) for t in terms]
    hbm, vmem = pl.BlockSpec(memory_space=pltpu.HBM), pl.BlockSpec(memory_space=pltpu.VMEM)
    dma = lambda *shape: pltpu.SemaphoreType.DMA(shape)
    return pl.pallas_call(
        functools.partial(_finish, layers=layers, count=sum(t.size for t in terms)),
        in_specs=[hbm] * (len(terms) + len(comes)),
        out_specs=[vmem] * 6,
        out_shape=[jax.ShapeDtypeStruct((layers, *m), BF16) for m in mine[:5]] + [jax.ShapeDtypeStruct((8, HEAD), F32)],
        scratch_shapes=[pltpu.VMEM(m, BF16) for m in mine] + [pltpu.VMEM((n - 1, *m), BF16) for m in mine] + [pltpu.VMEM((n, 8, HEAD), F32)]
        + [dma(len(terms))] * 2 + [dma(n - 1)] * 4,
        compiler_params=pltpu.CompilerParams(vmem_limit_bytes=VMEM, collective_id=number, has_side_effects=True),
    )(*terms, *comes)


def _adamw(*refs):
    factor = refs[0][:1, :1]
    grads, w, m, v, outs = refs[1:6], refs[6:13], refs[13:20], refs[20:27], refs[27:]
    at = 0
    for i in range(7):
        columns = w[i].shape[2]
        g = grads[0][0, :, at : at + columns] if i < 3 else grads[i - 2][0]
        at += columns
        g = g.astype(F32) * factor
        wide = w[i][0].astype(F32)
        new_m = 0.9 * m[i][0] + 0.1 * g
        new_v = 0.95 * v[i][0] + 0.05 * g * g
        outs[i][0] = (wide - 0.02 * (new_m * lax.rsqrt(new_v + 1e-8) + 0.1 * wide)).astype(BF16)
        outs[7 + i][0] = new_m
        outs[14 + i][0] = new_v


def adamw(factor, grads, weights, m, v):
    parts = 2
    tile = lambda a: (a, (1, a.shape[1] // parts, a.shape[2]), lambda i, j: (i, j, 0))
    out = lambda a: (a.shape, a.dtype, *tile(a)[1:])
    return _call(_adamw, (weights[0].shape[0], parts), [(factor, None)] + [tile(a) for a in (*grads, *weights, *m, *v)],
                 [out(a) for a in (*weights, *m, *v)], [], 20 * sum(a.size for a in m))


def solution(mesh):
    def step(x, dy, *arrays):
        weights, m, v = (arrays[i : i + 7] for i in (0, 7, 14))
        layers = weights[0].shape[0]
        wq, wk, wv, wo, w_gate, w_up, w_down = weights
        ids = itertools.count()
        e, f, ff = wq.shape[2], wk.shape[2], w_gate.shape[2]

        def qkv_of(n, when, parts):
            step = e // parts
            first = [(wq, n, at, step, 0, at, when) for at in range(0, e, step)]
            return [*first, (wk, n, 0, f, 0, e, when), (wv, n, 0, f, 0, e + f, when)]

        h = x[0]
        cos, sin = tables(h.shape[0], HEAD)
        kept = []
        (w_qkv,) = alone(Gather(next(ids), qkv_of(0, -1, 3)))
        for n in range(layers):
            q, k, val = qkv(h, w_qkv, cos, sin)
            fetch = Gather(next(ids), [(wo, n, 0, wo.shape[2], 0, 0, 5), (w_gate, n, 0, ff, 1, 0, 6), (w_up, n, 0, ff, 1, ff, 7),
                                       (w_down, n, 0, w_down.shape[2], 2, 0, -1)])
            o, lse, w_o, w_gu, w_d = attend(q, k, val, fetch)
            kept.append([h, q, k, val, o, lse, None, w_qkv, w_o, w_gu, w_d])
            if n < layers - 1:
                h2, h, w_qkv = mlp(h, o, w_o, w_gu, w_d, Gather(next(ids), qkv_of(n + 1, 3, 1)))
                kept[n][6] = h2

        by_h, terms, comes, left = dy[0], [None] * layers, [None] * layers, []
        for n in reversed(range(layers)):
            h, q, k, val, o, lse, h2, w_qkv, w_o, w_gu, w_d = kept[n]
            last = n == layers - 1
            beside = Scatter(next(ids), left) if left else None
            by_h, by_g, by_u, by_d, *come = mlp_back(h if last else h2, by_h, w_gu, w_d, beside, *((o, w_o) if last else ()))
            if left:
                comes[n + 1] = come + comes[n + 1]
            do, delta, by_o = out_back(by_h, w_o, o)
            now = ([by_o] if n == 0 else []) + [by_g, by_u, by_d]
            dq, dk, dv, *comes[n] = attend_back(q, k, val, do, lse, delta, cos, sin, Scatter(next(ids), now))
            by_h, by_qkv = qkv_back(h, by_h, dq, dk, dv, cos, sin, w_qkv)
            left = [by_qkv, by_o]
            terms[n] = [by_qkv, by_o, by_g, by_u, by_d]
        *grads, factor = finish(next(ids), sum(terms, []), sum(comes, []), layers)
        return tuple(adamw(factor, grads, weights, m, v))

    states, cut = P(("rep", "dp"), None, None), P(None, "dp", None)
    return jax.shard_map(
        step,
        mesh=mesh,
        in_specs=(states, states) + (cut,) * 21,
        out_specs=(P("rep", "dp", None),) * 21,
        check_vma=False,
    )
```

```python
import functools
import itertools

import jax
import jax.numpy as jnp
import numpy as np
from jax import lax
from jax.experimental import pallas as pl
from jax.experimental.pallas import tpu as pltpu
from jax.sharding import PartitionSpec as P

HEAD = 128
THETA = 10000
NAMES = ("wq", "wk", "wv", "wo", "w_gate", "w_up", "w_down")
NEG = -1e30
HIDDEN = 2 * NEG
LOG2E = 1.4426950408889634
VMEM = 60 * 2**20
F32, BF16 = jnp.float32, jnp.bfloat16


def _rows(i):
    return i, 0


def _columns(i):
    return 0, i


def _middle(i):
    return 0, i, 0


def _fixed(i):
    return 0, 0


def _first():
    return pl.program_id(0) == 0


def _last():
    return pl.program_id(0) == pl.num_programs(0) - 1


def _mm(a, b, ca=1, cb=0):
    return lax.dot_general(a, b, (((ca,), (cb,)), ((), ())), preferred_element_type=F32)


def _mt(a, b):
    return _mm(a, b, 1, 1)


def _fit(size, want, unit=128):
    return max(n for n in range(unit, max(min(want, size), unit) + 1, unit) if size % n == 0)


def _normed(h):
    wide = h.astype(F32)
    scale = lax.rsqrt(jnp.mean(wide * wide, -1, keepdims=True) + 1e-6)
    return wide, scale, (wide * scale).astype(BF16)


def _norm_back(wide, scale, by_a):
    by_a = by_a.astype(BF16).astype(F32)
    along = jnp.sum(by_a * wide, -1, keepdims=True) * (scale * scale * scale) * (1 / wide.shape[-1])
    return (by_a * scale - wide * along).astype(BF16)


def _plus(a, b):
    return (a.astype(F32) + b.astype(BF16).astype(F32)).astype(BF16)


def _turned(t, cos, sin):
    t = t.astype(BF16).astype(F32)
    return (t * cos + pltpu.roll(t, t.shape[1] // 2, 1) * sin).astype(BF16)


MESH = pl.DeviceIdType.MESH


class Gather:
    def __init__(self, number, pieces):
        self.number, self.pieces = number, pieces
        self.arrays = [p[0] for p in pieces]

    def ins(self):
        def block(n):
            return lambda *_: (n, 0, 0)

        return [(p[0], (1, *p[0].shape[1:]), block(p[1]), pl.Buffered(1)) for p in self.pieces]

    def outs(self, n):
        wholes = {}
        for a, _, _, width, whole, _, _ in self.pieces:
            wholes[whole] = (n * a.shape[1], wholes.get(whole, (0, 0))[1] + width)
        return [wholes[i] for i in range(len(wholes))]

    def scratch(self):
        return [pltpu.SemaphoreType.DMA((len(self.pieces), 3))] * 4 + [pltpu.SemaphoreType.DMA((len(self.pieces),))]

    def run(self, step, last, shards, wholes, scratch, before):
        send, come, give, get, own = scratch
        me, rep, n = lax.axis_index("dp"), lax.axis_index("rep"), lax.axis_size("dp")
        core = lax.rem(rep, 2)
        partner = rep + 1 - 2 * core
        place = [(wholes[p[4]], pl.ds(p[2], p[3]), pl.ds(p[5], p[3]), p[0].shape[1] // 2) for p in self.pieces]

        def rows(half, owner, which):
            return pl.ds(pl.multiple_of((2 * owner + which) * half, half), half)

        def out(i, d):
            whole, cols, at, half = place[i]
            return pltpu.make_async_remote_copy(
                src_ref=shards[i].at[0, rows(half, 0, core), cols], dst_ref=whole.at[rows(half, me, core), at],
                send_sem=send.at[i, d - 1], recv_sem=come.at[i, d - 1], device_id={"dp": lax.rem(me + d, n)}, device_id_type=MESH)

        def over(i, d):
            whole, _, at, half = place[i]
            where = rows(half, lax.rem(me + n - d, n), core)
            return pltpu.make_async_remote_copy(
                src_ref=whole.at[where, at], dst_ref=whole.at[where, at],
                send_sem=give.at[i, d - 1], recv_sem=get.at[i, d - 1], device_id={"rep": partner}, device_id_type=MESH)

        def mine(i):
            whole, cols, at, half = place[i]
            return pltpu.make_async_copy(shards[i].at[0, :, cols], whole.at[pl.ds(pl.multiple_of(me * 2 * half, 2 * half), 2 * half), at], own.at[i])

        count = len(self.pieces)
        all_ = [(i, d) for i in range(count) for d in range(1, n)]
        if before:

            @pl.when(step == 0)
            def _():
                barrier = pltpu.get_barrier_semaphore()
                for d in range(1, n):
                    pl.semaphore_signal(barrier, inc=1, device_id={"dp": lax.rem(me + d, n)}, device_id_type=MESH)
                pl.semaphore_signal(barrier, inc=1, device_id={"rep": partner}, device_id_type=MESH)
                pl.semaphore_wait(barrier, n)
                for i, d in all_:
                    out(i, d).start()
                for i in range(count):
                    mine(i).start()

        for when in sorted({p[6] for p in self.pieces}):
            if before == (when >= 0):

                @pl.when(step == (when if when >= 0 else last))
                def _():
                    for i, d in all_:
                        if self.pieces[i][6] == when:
                            out(i, d).wait_recv()
                            over(i, d).start()

        if not before:

            @pl.when(step == last)
            def _():
                for i, d in all_:
                    out(i, d).wait_send()
                    over(i, d).wait()
                for i in range(count):
                    mine(i).wait()


class Scatter:
    def __init__(self, number, pieces):
        self.number, self.pieces = number, pieces
        self.arrays = [p[0] for p in pieces]

    def ins(self):
        return [(a, pltpu.HBM) for a in self.arrays]

    def outs(self, n):
        return [(n - 1, a.shape[0] // n, width) for a, _, width in self.pieces]

    def scratch(self):
        return [pltpu.SemaphoreType.DMA((len(self.arrays), 3))] * 2

    def run(self, step, last, terms, comes, scratch, before):
        send, come = scratch
        me, n = lax.axis_index("dp"), lax.axis_size("dp")

        def out(i, d):
            to = lax.rem(me + d, n)
            size = terms[i].shape[0] // n
            columns = pl.ds(self.pieces[i][1], self.pieces[i][2])
            return pltpu.make_async_remote_copy(
                src_ref=terms[i].at[pl.ds(pl.multiple_of(to * size, size), size), columns], dst_ref=comes[i].at[d - 1],
                send_sem=send.at[i, d - 1], recv_sem=come.at[i, d - 1], device_id={"dp": to}, device_id_type=MESH)

        all_ = [(i, d) for i in range(len(terms)) for d in range(1, n)]

        if before:

            @pl.when(step == 0)
            def _():
                barrier = pltpu.get_barrier_semaphore()
                for d in range(1, n):
                    pl.semaphore_signal(barrier, inc=1, device_id={"dp": lax.rem(me + d, n)}, device_id_type=MESH)
                pl.semaphore_wait(barrier, n - 1)
                for i, d in all_:
                    out(i, d).start()

        else:

            @pl.when(step == last)
            def _():
                for i, d in all_:
                    out(i, d).wait()


def _call(kernel, grid, ins, outs, scratch, flops, exp=0, beside=None):
    whole = lambda a: pl.BlockSpec(a.shape, lambda *_: (0,) * a.ndim, pipeline_mode=pl.Buffered(1))
    spec = lambda i: whole(i[0]) if i[1] is None else pl.BlockSpec(memory_space=i[1]) if i[1] is pltpu.HBM else pl.BlockSpec(i[1], i[2], pipeline_mode=i[3] if len(i) > 3 else None)
    size = sum(i[0].size * i[0].dtype.itemsize for i in ins)
    out_specs = [pl.BlockSpec(o[2], o[3]) for o in outs]
    shapes = [jax.ShapeDtypeStruct(o[0], o[1]) for o in outs]
    body, more = kernel, {}
    if beside is not None:
        more = dict(collective_id=beside.number, has_side_effects=True)
        wholes = beside.outs(lax.axis_size("dp"))
        counts = [len(ins), len(beside.arrays), len(outs), len(wholes), len(scratch)]
        ins = ins + beside.ins()
        shapes += [jax.ShapeDtypeStruct(o, BF16) for o in wholes]
        out_specs += [pl.BlockSpec(memory_space=pltpu.HBM)] * len(wholes)
        scratch = scratch + beside.scratch()

        def body(*refs):
            split, at = [], 0
            for c in counts:
                split.append(refs[at : at + c])
                at += c
            step, last = pl.program_id(0), pl.num_programs(0) - 1
            beside.run(step, last, split[1], split[3], refs[at:], True)
            kernel(*split[0], *split[2], *split[4])
            beside.run(step, last, split[1], split[3], refs[at:], False)

    return pl.pallas_call(
        body,
        grid=grid,
        in_specs=[spec(i) for i in ins],
        out_specs=out_specs,
        out_shape=shapes,
        scratch_shapes=scratch,
        compiler_params=pltpu.CompilerParams(dimension_semantics=("arbitrary",) * len(grid), vmem_limit_bytes=VMEM, **more),
        cost_estimate=pl.CostEstimate(flops=flops, transcendentals=exp, bytes_accessed=2 * size),
    )(*[i[0] for i in ins])


def alone(beside):
    return _call(lambda: None, (1,), [], [], [], 0, beside=beside)


def _qkv(h_ref, w_ref, cos_ref, sin_ref, q_ref, k_ref, v_ref):
    a = _normed(h_ref[:])[2]
    cos, sin = cos_ref[:], sin_ref[:]
    heads = q_ref.shape[0]
    for n in range(0, heads + 2, 2):
        y = _mm(a, w_ref[:, n * HEAD : (n + 2) * HEAD])
        for at in range(n, n + 2):
            part = y[:, (at - n) * HEAD : (at - n + 1) * HEAD]
            if at < heads:
                q_ref[at] = _turned(part, cos, sin)
            elif at == heads:
                k_ref[:] = _turned(part, cos, sin)
            else:
                v_ref[:] = part.astype(BF16)


def qkv(h, w, cos, sin, beside=None):
    t, d = h.shape
    heads = w.shape[1] // HEAD - 2
    bt = _fit(t, 512)
    rows = _rows
    return _call(
        _qkv, (t // bt,),
        [(h, (bt, d), rows), (w, None), (cos, (bt, HEAD), rows), (sin, (bt, HEAD), rows)],
        [((heads, t, HEAD), BF16, (heads, bt, HEAD), _middle), ((t, HEAD), BF16, (bt, HEAD), rows), ((t, HEAD), BF16, (bt, HEAD), rows)],
        [], 2 * t * d * w.shape[1], 0, beside,
    )


def _spans(iq, bq, bk, block):
    lax.fori_loop(0, lax.div(iq * bq, bk), lambda j, _: block(j * bk, bk, False), None)
    rest = lax.rem(iq, bk // bq)
    for n in range(bk // bq):

        @pl.when(rest == n)
        def _():
            block((iq - n) * bq, (n + 1) * bq, True)


def _level(size, wide, bq):
    return (lax.broadcasted_iota(jnp.int32, (size, wide), 0) - lax.rem(lax.broadcasted_iota(jnp.int32, (size, wide), 1), bq)) <= size - bq


def _attend(q_ref, k_ref, v_ref, o_ref, lse_ref, top_s, mix_s, *, bk, wide):
    g, bq, d = q_ref.shape
    cols = g * bq
    iq = pl.program_id(0)
    scale = d**-0.5
    e = scale * LOG2E
    pieces = range(0, cols, wide)
    top_s[:] = jnp.full((1, cols), NEG, F32)
    mix_s[:] = jnp.zeros((d + 8, cols), F32)

    def block(at_key, size, masked):
        here = pl.ds(pl.multiple_of(at_key, bq), size)
        keys = k_ref[here, :]
        values = jnp.concatenate([v_ref[here, :].T, jnp.ones((8, size), BF16)], axis=0)
        scores = [_mt(keys, q_ref[:].reshape(cols, d)[at : at + wide, :]) for at in pieces]
        ok = _level(size, wide, bq) if masked else None
        weights, keeps = [], []
        for at, s in zip(pieces, scores):
            if masked:
                s = jnp.where(ok, s, HIDDEN)
            old = top_s[:, at : at + wide]
            top = jnp.maximum(old, s.max(axis=0, keepdims=True))
            top_s[:, at : at + wide] = top
            weights.append(jnp.exp2((s - top) * e).astype(BF16))
            keeps.append(jnp.exp2((old - top) * e))
        for at, p, keep in zip(pieces, weights, keeps):
            mix_s[:, at : at + wide] = mix_s[:, at : at + wide] * keep + _mm(values, p)

    _spans(iq, bq, bk, block)
    for n in range(g):
        at = slice(n * bq, (n + 1) * bq)
        total = mix_s[d : d + 1, at]
        o_ref[:, n * d : (n + 1) * d] = (mix_s[:d, at] * (1 / total)).T.astype(BF16)
        lse_ref[n : n + 1, :] = top_s[:, at] * scale + jnp.log(total)


def attend(q, k, v, beside):
    g, t, d = q.shape
    bq = _fit(t, 256)
    bk = _fit(t, 1024)
    wide = _fit(g * bq, 512, bq)
    rows = _rows
    return _call(
        functools.partial(_attend, bk=bk, wide=wide), (t // bq,),
        [(q, (g, bq, d), _middle), (k, None), (v, None)],
        [((t, g * d), BF16, (bq, g * d), rows), ((g, t), F32, (g, bq), _columns)],
        [pltpu.VMEM((1, g * bq), F32), pltpu.VMEM((d + 8, g * bq), F32)],
        2 * g * t * t * d, g * t * t // 2, beside,
    )


def _out_back(by_h_ref, wo_ref, o_ref, do_ref, delta_ref, by_w_ref, sum_s):
    by_h = by_h_ref[:]
    heads = o_ref.shape[1] // HEAD

    @pl.when(_first())
    def _():
        sum_s[:] = jnp.zeros_like(sum_s)

    for n in range(0, heads, 2):
        at = slice(n * HEAD, (n + 2) * HEAD)
        do = _mt(by_h, wo_ref[at, :]).astype(BF16)
        do_ref[:, at] = do
        o = o_ref[:, at]
        both = do.astype(F32) * o.astype(F32)
        for m in range(2):
            delta_ref[n + m : n + m + 1, :] = both[:, m * HEAD : (m + 1) * HEAD].T.sum(axis=0, keepdims=True)
        sum_s[at, :] += _mm(o.T, by_h)

    @pl.when(_last())
    def _():
        by_w_ref[:] = sum_s[:].astype(BF16)


def out_back(by_h, wo, o, beside=None):
    t, d = by_h.shape
    wide = o.shape[1]
    bt = _fit(t, 512)
    rows = _rows
    return _call(
        _out_back, (t // bt,),
        [(by_h, (bt, d), rows), (wo, None), (o, (bt, wide), rows)],
        [((t, wide), BF16, (bt, wide), rows), ((wide // HEAD, t), F32, (wide // HEAD, bt), _columns), (wo.shape, BF16, wo.shape, _fixed)],
        [pltpu.VMEM(wo.shape, F32)], 4 * t * wo.size, 0, beside,
    )


def _attend_back(q_ref, k_ref, v_ref, do_ref, lse_ref, delta_ref, cos_ref, sin_ref, dq_ref, dk_ref, dv_ref, dq_s, dk_s, dv_s, *, bk, wide):
    g, bq, d = q_ref.shape
    cols = g * bq
    iq = pl.program_id(0)
    scale = d**-0.5
    e = scale * LOG2E
    per = wide // bq
    pieces = range(0, cols, wide)

    @pl.when(_first())
    def _():
        dk_s[:] = jnp.zeros_like(dk_s)
        dv_s[:] = jnp.zeros_like(dv_s)

    dq_s[:] = jnp.zeros_like(dq_s)
    lses = jnp.concatenate([lse_ref[n : n + 1, :] for n in range(g)], axis=1) * LOG2E
    deltas = jnp.concatenate([delta_ref[n : n + 1, :] for n in range(g)], axis=1)

    def block(at_key, size, masked):
        here = pl.ds(pl.multiple_of(at_key, bq), size)
        keys, values = k_ref[here, :], v_ref[here, :]
        turned = keys.T
        qs = [q_ref[:].reshape(cols, d)[at : at + wide, :] for at in pieces]
        dos = [jnp.concatenate([do_ref[:, (n + at // bq) * d : (n + at // bq + 1) * d] for n in range(per)], axis=0) for at in pieces]
        scores = [_mt(keys, x) for x in qs]
        dps = [_mt(values, x) for x in dos]
        ok = _level(size, wide, bq) if masked else None
        for n, at in enumerate(pieces):
            p = jnp.exp2(scores[n] * e - lses[:, at : at + wide])
            if masked:
                p = jnp.where(ok, p, 0.0)
            ds = (p * (dps[n] - deltas[:, at : at + wide])).astype(BF16)
            dv_s[here, :] += _mm(p.astype(BF16), dos[n])
            dk_s[here, :] += _mm(ds, qs[n])
            dq_s[:, at : at + wide] += _mm(turned, ds)

    _spans(iq, bq, bk, block)
    cos, sin = cos_ref[:], -sin_ref[:]
    for n in range(g):
        dq_ref[:, n * d : (n + 1) * d] = _turned((dq_s[:, n * bq : (n + 1) * bq] * scale).T, cos, sin)

    @pl.when(_last())
    def _():
        dk_ref[:] = (dk_s[:] * scale).astype(BF16)
        dv_ref[:] = dv_s[:].astype(BF16)


def attend_back(q, k, v, do, lse, delta, cos, sin, beside):
    g, t, d = q.shape
    bq = _fit(t, 256)
    bk = _fit(t, 512)
    wide = _fit(g * bq, 512, bq)
    rows = _rows
    stats = ((g, bq), _columns)
    return _call(
        functools.partial(_attend_back, bk=bk, wide=wide), (t // bq,),
        [(q, (g, bq, d), _middle), (k, None), (v, None), (do, (bq, g * d), rows), (lse, *stats), (delta, *stats),
         (cos, (bq, d), rows), (sin, (bq, d), rows)],
        [((t, g * d), BF16, (bq, g * d), rows), (k.shape, BF16, k.shape, _fixed), (v.shape, BF16, v.shape, _fixed)],
        [pltpu.VMEM((d, g * bq), F32), pltpu.VMEM(k.shape, F32), pltpu.VMEM(v.shape, F32)],
        5 * g * t * t * d, g * t * t // 2, beside,
    )


def _qkv_back(h_ref, dq_ref, dk_ref, dv_ref, cos_ref, sin_ref, *refs):
    by_h_ref, w_ref, out_ref, by_w_ref, sum_s = refs if len(refs) == 5 else (None, None, None, *refs)
    wide, scale, a = _normed(h_ref[:])
    at = a.T

    @pl.when(_first())
    def _():
        sum_s[:] = jnp.zeros_like(sum_s)

    heads = dq_ref.shape[1] // HEAD
    rest = jnp.concatenate([_turned(dk_ref[:], cos_ref[:], -sin_ref[:]), dv_ref[:]], axis=1)
    by_a = jnp.zeros(wide.shape, F32)
    for n in range(0, heads + 2, 2):
        here = slice(n * HEAD, (n + 2) * HEAD)
        g = dq_ref[:, here] if n < heads else rest
        if by_h_ref is not None:
            by_a = by_a + _mt(g, w_ref[:, here])
        sum_s[:, here] += _mm(at, g)
    if by_h_ref is not None:
        out_ref[:] = _plus(by_h_ref[:], _norm_back(wide, scale, by_a))

    @pl.when(_last())
    def _():
        by_w_ref[:] = sum_s[:].astype(BF16)


def qkv_back(h, dq, dk, dv, cos, sin, columns, by_h=None, w=None, beside=None):
    t, d = h.shape
    bt = _fit(t, 512)
    rows = _rows
    tile = lambda a: (a, (bt, a.shape[1]), rows)
    states = by_h is not None
    return _call(
        _qkv_back, (t // bt,),
        [tile(a) for a in (h, dq, dk, dv, cos, sin)] + ([tile(by_h), (w, None)] if states else []),
        ([(h.shape, BF16, (bt, d), rows)] if states else []) + [((d, columns), BF16, (d, columns), _fixed)],
        [pltpu.VMEM((d, columns), F32)], 4 * t * d * columns, 0, beside,
    )


def _mlp(h_ref, o_ref, wo_ref, gu_ref, down_ref, h2_ref, y_ref, gate_ref, up_ref, *, chunk):
    h2 = _plus(h_ref[:], _mm(o_ref[:], wo_ref[:]))
    h2_ref[:] = h2
    b = _normed(h2)[2]
    ff = down_ref.shape[0]
    y = jnp.zeros(h_ref.shape, F32)
    for c in range(0, ff, chunk):
        gate = _mm(b, gu_ref[:, c : c + chunk])
        up = _mm(b, gu_ref[:, ff + c : ff + c + chunk])
        gate_ref[:, c : c + chunk] = gate
        up_ref[:, c : c + chunk] = up
        y = y + _mm((gate * jax.nn.sigmoid(gate) * up).astype(BF16), down_ref[c : c + chunk, :])
    y_ref[:] = _plus(h2, y)


def mlp(h, o, wo, gu, down, beside):
    t, d = h.shape
    bt = _fit(t, 512)
    rows = _rows
    return _call(
        functools.partial(_mlp, chunk=_fit(down.shape[0], 512)), (t // bt,),
        [(h, (bt, d), rows), (o, (bt, o.shape[1]), rows), (wo, None), (gu, None), (down, None)], [(h.shape, BF16, (bt, d), rows)] * 2 + [((t, down.shape[0]), F32, (bt, down.shape[0]), rows)] * 2, [],
        2 * t * (wo.size + gu.size + down.size), t * down.shape[0], beside,
    )


def _mlp_back(*refs, chunk, project):
    first, second, *refs = refs
    if project:
        o_ref, wo_ref = first, second
    h_ref, dy_ref, gu_ref, down_ref, out_ref, by_gate_ref, by_up_ref, by_down_ref, gu_s, down_s = refs
    wide, scale, b = _normed(_plus(h_ref[:], _mm(o_ref[:], wo_ref[:])) if project else h_ref[:])
    bt = b.T
    dy = dy_ref[:]
    ff = down_ref.shape[0]

    @pl.when(_first())
    def _():
        gu_s[:] = jnp.zeros_like(gu_s)
        down_s[:] = jnp.zeros_like(down_s)

    by_b = jnp.zeros(wide.shape, F32)
    for c in range(0, ff, chunk):
        g, u = slice(c, c + chunk), slice(ff + c, ff + c + chunk)
        gate, up = (_mm(b, gu_ref[:, g]), _mm(b, gu_ref[:, u])) if project else (first[:, g], second[:, g])
        by = _mt(dy, down_ref[g, :]).astype(BF16).astype(F32)
        part = jax.nn.sigmoid(gate)
        silu = gate * part
        by_up = (by * silu).astype(BF16)
        by_gate = (by * up * (part * (1 + gate * (1 - part)))).astype(BF16)
        down_s[g, :] += _mm((silu * up).astype(BF16).T, dy)
        by_b = by_b + _mt(by_gate, gu_ref[:, g]) + _mt(by_up, gu_ref[:, u])
        gu_s[:, g] += _mm(bt, by_gate)
        gu_s[:, u] += _mm(bt, by_up)
    out_ref[:] = _plus(dy, _norm_back(wide, scale, by_b))

    @pl.when(_last())
    def _():
        by_gate_ref[:] = gu_s[:, :ff].astype(BF16)
        by_up_ref[:] = gu_s[:, ff:].astype(BF16)
        by_down_ref[:] = down_s[:].astype(BF16)


def mlp_back(h, dy, gu, down, beside, first, second, project):
    t, d = h.shape
    bt = _fit(t, 512)
    rows = _rows
    return _call(
        functools.partial(_mlp_back, chunk=_fit(down.shape[0], 512), project=project), (t // bt,),
        [(first, (bt, first.shape[1]), rows), (second, None) if project else (second, (bt, second.shape[1]), rows)] + [(h, (bt, d), rows), (dy, (bt, d), rows), (gu, None), (down, None)],
        [(h.shape, BF16, (bt, d), rows), *[((d, down.shape[0]), BF16, (d, down.shape[0]), _fixed)] * 2, (down.shape, BF16, down.shape, _fixed)],
        [pltpu.VMEM(gu.shape, F32), pltpu.VMEM(down.shape, F32)], 6 * t * (gu.size + down.size), t * down.shape[0], beside,
    )


def tables(t, head):
    half = head // 2
    angle = np.arange(t, dtype=np.float32)[:, None] * (np.float32(THETA) ** (-np.arange(half, dtype=np.float32) / np.float32(half)))
    cos, sin = (f(angle.astype(np.float64)).astype(np.float32) for f in (np.cos, np.sin))
    return jnp.asarray(np.concatenate([cos, cos], 1)), jnp.asarray(np.concatenate([-sin, sin], 1))


def _finish(*refs, layers, count, places):
    sizes, split, at = [layers * 5, len(places), 5, 1, layers * 5, layers * 5], [], 0
    for size in sizes:
        split.append(refs[at : at + size])
        at += size
    terms, comes, outs, (factor_ref,), own, come = split
    squares_s, here_sem, come_sem, send, get, send_sum, get_sum = refs[at:]
    me, n = lax.axis_index("dp"), lax.axis_size("dp")
    barrier = pltpu.get_barrier_semaphore()
    for d in range(1, n):
        pl.semaphore_signal(barrier, inc=1, device_id={"dp": lax.rem(me + d, n)}, device_id_type=MESH)
    pl.semaphore_wait(barrier, n - 1)

    def rows(i, owner):
        size = own[i].shape[0]
        return pl.ds(pl.multiple_of(owner * size, size), size)

    def out(d):
        to = lax.rem(me + d, n)
        return pltpu.make_async_remote_copy(src_ref=terms[0].at[rows(0, to), :], dst_ref=come[0].at[d - 1], send_sem=send.at[d - 1], recv_sem=get.at[d - 1],
                                            device_id={"dp": to}, device_id_type=MESH)

    for d in range(1, n):
        out(d).start()
    local = lambda i: pltpu.make_async_copy(terms[i].at[rows(i, me), :], own[i], here_sem.at[i])
    came = lambda j: pltpu.make_async_copy(comes[j], come[places[j][0]].at[:, :, pl.ds(places[j][1], comes[j].shape[2])], come_sem.at[j])
    parts = lambda i: [j for j in range(len(places)) if places[j][0] == i]
    for i in [*range(1, layers * 5), 0]:
        local(i).start()
        for j in parts(i):
            came(j).start()

    def total(i):
        size, columns = own[i].shape
        part = 16

        def some(j, squares):
            here = pl.ds(pl.multiple_of(j * part, part), part)
            g = own[i][here, :].astype(F32)
            for d in range(n - 1):
                g = g + come[i][d, here, :].astype(F32)
            g = g.astype(BF16)
            outs[i % 5][i // 5, here, :] = g
            g = g.astype(F32)
            g = g * g
            g = sum(g[:, c : c + HEAD] for c in range(0, columns, HEAD))
            return squares + g[:8] + g[8:]

        return lax.fori_loop(0, size // part, some, jnp.zeros((8, HEAD), F32))

    squares = jnp.zeros((8, HEAD), F32)
    for i in range(1, layers * 5):
        local(i).wait()
        for j in parts(i):
            came(j).wait()
        squares = squares + total(i)
    local(0).wait()
    for d in range(1, n):
        out(d).wait()
    squares_s[0] = squares + total(0)

    def tell(d):
        return pltpu.make_async_remote_copy(src_ref=squares_s.at[0], dst_ref=squares_s.at[d], send_sem=send_sum.at[d - 1], recv_sem=get_sum.at[d - 1],
                                            device_id={"dp": lax.rem(me + d, n)}, device_id_type=MESH)

    for d in range(1, n):
        tell(d).start()
    for d in range(1, n):
        tell(d).wait()
    all_ = jnp.zeros((8, HEAD), F32)
    for owner in range(n):
        all_ = all_ + squares_s[lax.rem(me + n - owner, n)]
    both = jnp.sum(jnp.sum(all_, axis=1, keepdims=True), axis=0, keepdims=True)
    factor_ref[:] = jnp.broadcast_to(jnp.minimum(1.0, 0.5 * lax.rsqrt(both / count + 1e-30)), factor_ref.shape)


def finish(number, terms, comes, places, layers):
    n = lax.axis_size("dp")
    mine = [(t.shape[0] // n, t.shape[1]) for t in terms]
    hbm, vmem = pl.BlockSpec(memory_space=pltpu.HBM), pl.BlockSpec(memory_space=pltpu.VMEM)
    dma = lambda *shape: pltpu.SemaphoreType.DMA(shape)
    return pl.pallas_call(
        functools.partial(_finish, layers=layers, count=sum(t.size for t in terms), places=places),
        in_specs=[hbm] * (len(terms) + len(comes)),
        out_specs=[vmem] * 6,
        out_shape=[jax.ShapeDtypeStruct((layers, *m), BF16) for m in mine[:5]] + [jax.ShapeDtypeStruct((8, HEAD), F32)],
        scratch_shapes=[pltpu.VMEM(m, BF16) for m in mine] + [pltpu.VMEM((n - 1, *m), BF16) for m in mine] + [pltpu.VMEM((n, 8, HEAD), F32)]
        + [dma(len(terms)), dma(len(comes))] + [dma(n - 1)] * 4,
        compiler_params=pltpu.CompilerParams(vmem_limit_bytes=VMEM, collective_id=number, has_side_effects=True),
    )(*terms, *comes)


def _adamw(*refs):
    factor = refs[0][:1, :1]
    grads, w, m, v, outs = refs[1:6], refs[6:13], refs[13:20], refs[20:27], refs[27:]
    at = 0
    for i in range(7):
        columns = w[i].shape[2]
        g = grads[0][0, :, at : at + columns] if i < 3 else grads[i - 2][0]
        at += columns
        g = g.astype(F32) * factor
        wide = w[i][0].astype(F32)
        new_m = 0.9 * m[i][0] + 0.1 * g
        new_v = 0.95 * v[i][0] + 0.05 * g * g
        outs[i][0] = (wide - 0.02 * (new_m * lax.rsqrt(new_v + 1e-8) + 0.1 * wide)).astype(BF16)
        outs[7 + i][0] = new_m
        outs[14 + i][0] = new_v


def adamw(factor, grads, weights, m, v):
    parts = 2
    tile = lambda a: (a, (1, a.shape[1] // parts, a.shape[2]), lambda i, j: (i, j, 0))
    out = lambda a: (a.shape, a.dtype, *tile(a)[1:])
    return _call(_adamw, (weights[0].shape[0], parts), [(factor, None)] + [tile(a) for a in (*grads, *weights, *m, *v)],
                 [out(a) for a in (*weights, *m, *v)], [], 20 * sum(a.size for a in m))


def solution(mesh):
    def step(x, dy, *arrays):
        weights, m, v = (arrays[i : i + 7] for i in (0, 7, 14))
        layers = weights[0].shape[0]
        wq, wk, wv, wo, w_gate, w_up, w_down = weights
        ids = itertools.count()
        e, f, ff = wq.shape[2], wk.shape[2], w_gate.shape[2]

        def cut(w, n, whole, at, whens):
            ends = [w.shape[2] * p // len(whens) // HEAD * HEAD for p in range(len(whens) + 1)]
            return [(w, n, a, b - a, whole, at + a, when) for a, b, when in zip(ends, ends[1:], whens)]

        def qkv_of(n, *whens):
            return [*cut(wq, n, 0, 0, whens), *cut(wk, n, 0, e, whens[-1:]), *cut(wv, n, 0, e + f, whens[-1:])]

        h = x[0]
        cos, sin = tables(h.shape[0], HEAD)
        kept = []
        (w_qkv,) = alone(Gather(next(ids), qkv_of(0, -1, -1, -1, -1)))
        for n in range(layers):
            q, k, val = qkv(h, w_qkv, cos, sin)
            pieces = [*cut(w_gate, n, 0, 0, (5, 6)), *cut(w_up, n, 0, ff, (6, 7)), *cut(w_down, n, 1, 0, (7, 7) if n else (-1, -1))]
            o, lse, w_gu, w_d, *got = attend(q, k, val, Gather(next(ids), pieces if n else cut(wo, n, 2, 0, (4, 5)) + pieces))
            w_o = got[0] if got else w_o
            kept.append([h, q, k, val, o, lse, None, w_qkv, w_o, w_gu, w_d])
            if n < layers - 1:
                h2, h, gate, up, w_qkv, w_o = mlp(h, o, w_o, w_gu, w_d, Gather(next(ids), qkv_of(n + 1, 1, 2) + cut(wo, n + 1, 1, 0, (3, 3))))
                kept[n][6] = h2, gate, up

        by_h, terms, comes, places = dy[0], [None] * (5 * layers), [], []

        def carried(*pieces):
            places.extend((i, at) for i, at, _ in pieces)
            return Scatter(next(ids), [(terms[i], at, width) for i, at, width in pieces])

        whole = lambda i: (i, 0, terms[i].shape[1])
        part = _fit(wo.shape[2], wo.shape[2] * 3 // 5)
        for n in reversed(range(layers)):
            h, q, k, val, o, lse, saved, w_qkv, w_o, w_gu, w_d = kept[n]
            at, last = 5 * n, n == layers - 1
            beside = None if last else carried(whole(at + 5), (at + 6, part, wo.shape[2] - part))
            given = (o, w_o, True) if last else (*saved[1:], False)
            by_h, by_gate, by_up, by_down, *come = mlp_back(h if last else saved[0], by_h, w_gu, w_d, beside, *given)
            terms[at + 2 : at + 5] = by_gate, by_up, by_down
            comes += come
            early = ff // 2 if n == 0 else 0
            do, delta, terms[at + 1], *come = out_back(by_h, w_o, o, carried((at + 2, 0, early)) if early else None)
            comes += come
            now = [(at + 2, early, ff - early), whole(at + 3), whole(at + 4)] + ([whole(at + 1)] if n == 0 else [])
            dq, dk, dv, *come = attend_back(q, k, val, do, lse, delta, cos, sin, carried(*now))
            comes += come
            if n:
                by_h, terms[at], *come = qkv_back(h, dq, dk, dv, cos, sin, w_qkv.shape[1], by_h, w_qkv, carried((at + 1, 0, part)))
                comes += come
            else:
                (terms[at],) = qkv_back(h, dq, dk, dv, cos, sin, w_qkv.shape[1])
        *grads, factor = finish(next(ids), terms, comes, places, layers)
        return tuple(adamw(factor, grads, weights, m, v))

    states, cut = P(("rep", "dp"), None, None), P(None, "dp", None)
    return jax.shard_map(
        step,
        mesh=mesh,
        in_specs=(states, states) + (cut,) * 21,
        out_specs=(P("rep", "dp", None),) * 21,
        check_vma=False,
    )
```
